256 devices in a mesh: band: 64 (over x, y, z_hi, core), chan: 4 (over z_lo).
Axes of the slice: x: 4, y: 4, z: 8 (z_hi: 2, z_lo: 4; z = z_hi * 4 + z_lo), core: 2. Of those that a mesh axis runs over, the one named last changes fastest.
Arguments:
- cells_next: bfloat16 [131072, 1024], P('band', 'chan'), may hold values from -6 to 6
- node_embed: bfloat16 [16384, 1024], P('band', 'chan'), may hold values from -6 to 6
- enc_mix: bfloat16 [1024, 1024], P(None, 'chan'), may hold values from -0.1875 to 0.1875
- out_cotangent: bfloat16 [131072, 1024], P('band', 'chan'), may hold values from -16 to 16
- decoded_saved: bfloat16 [131072, 1024], P('band', 'chan'), may hold values from -6 to 6
- dec_proj: bfloat16 [1024, 1024], P(None, 'chan'), may hold values from -0.1875 to 0.1875
- tile_source: int32 [128, 16], replicated, may hold values from 0 to 1023, as said below
- tile_codes: int32 [128, 16, 128, 128], P('band'), may hold values from 0 to 65535
Outputs:
- hidden_nodes: bfloat16 [16384, 1024], P('band', 'chan')
- node_grad: bfloat16 [16384, 1024], P('band', 'chan')
- w_dec_grad: float32 [1024, 1024], P('band', 'chan')
The draws below stay inside these ranges and needn't reach their ends.
Inputs may be any that keep to these rules, and one draw needn't show every extreme that they name: `tile_source`: each entry is a cell block; cell block c lies in band c // 16 and node block n in band n // 2. The cell blocks of a node block's tiles lie within 3 bands of its own. Of the 32 tiles of one band's node blocks, exactly 8 read that band itself and at most 8 read any other one band.
All inputs are finite; a program needn't handle non-finite values.
Results may differ from the reference program's by a relative error of at most 0.0049.
Values may be sent and summed in bfloat16 or wider, within the bound.
No kernel may reach another device: no remote copies, remote signals or barrier semaphores. Data moves between devices by JAX's collectives and lax.ppermute only.
A program may use at most 64 MiB of HBM per device.

```python
import jax
import jax.numpy as jnp
from jax import lax

D = 1024
BLK = 128
K = 16
R = 3
CB_DEV = 16
NB_DEV = 2
CAP = 8
NODE_BLOCKS = 128
CELLS = 131072
NODES = 16384


def draw_tile_source(key, part):
    band_total = NODE_BLOCKS // NB_DEV
    tile_total = NB_DEV * K
    pool_size = 2 * R * CAP

    def one_band(band_key, owner):
        score_key, shuffle_key, local_key = jax.random.split(band_key, 3)
        tokens = jnp.arange(pool_size, dtype=jnp.int32)
        neighbour = tokens // CAP
        offset = jnp.where(neighbour < R, neighbour - R, neighbour - R + 1)
        source = owner + offset
        usable = (source >= 0) & (source < band_total)
        scores = jax.random.randint(score_key, (pool_size,), 0, 1 << 20, dtype=jnp.int32) * pool_size + tokens
        scores = jnp.where(usable, scores, (1 << 30) + tokens)
        ranking = jnp.argsort(scores)
        picked = source[ranking[:tile_total - CAP]]
        bands_drawn = jnp.concatenate([jnp.full((CAP,), owner, jnp.int32), picked.astype(jnp.int32)])
        shuffle = jax.random.permutation(shuffle_key, tile_total)
        local_block = jax.random.randint(local_key, (tile_total,), 0, CB_DEV, dtype=jnp.int32)
        return (bands_drawn[shuffle] * CB_DEV + local_block).reshape(NB_DEV, K)
    band_keys = jax.random.split(key, band_total)
    drawn = jax.vmap(one_band)(band_keys, jnp.arange(band_total, dtype=jnp.int32))
    return drawn.reshape(band_total * NB_DEV, K).astype(jnp.int32)


def plant(array, rng, smallest, high):
    extent = array.shape
    place = [jax.random.randint(jax.random.fold_in(rng, axis), (), 0, extent[axis]) for axis in range(len(extent))]
    array = array.at[tuple(place)].set(smallest)
    longest = extent.index(max(extent))
    place[longest] = (place[longest] + 1) % extent[longest]
    return array.at[tuple(place)].set(high)


def spiked(result, own_key, source, target, shards_of, factor):
    owner, partner = [(jnp.arange(result.shape[position]) // (result.shape[position] // shards_of)).reshape([-1 if axis == position else 1 for axis in range(result.ndim)]) for position in (source, target)]
    chosen = jax.random.permutation(own_key, shards_of)[partner]
    strong = (owner == chosen) | (owner == (partner + shards_of // 2) % shards_of)
    return jnp.where(strong, factor * result, result)


def shard_levels(own_key, shape, shards, smallest, top_value):
    level = 1.0
    for axis_at, parts in shards:
        steps = jax.random.uniform(jax.random.fold_in(jax.random.fold_in(own_key, 6), axis_at), (parts,), jnp.float32, smallest / len(shards), top_value / len(shards))
        level = level * jnp.repeat(jnp.exp(steps), shape[axis_at] // parts).reshape((-1,) + (1,) * (len(shape) - 1 - axis_at))
    return level


def noise(rng, shape, scale, reach, shards=(), kind=jnp.bfloat16):
    values = scale * jax.random.normal(rng, shape, jnp.float32)
    if shards:
        values = values * shard_levels(rng, shape, shards, -0.22, 0.18)
    return jnp.clip(values, -reach, reach).astype(kind)


def heavy_noise(stream_key, extent, spread, limit, cuts, heavy, held_as=jnp.bfloat16):
    entries = spread * jax.random.normal(stream_key, extent, jnp.float32)
    if cuts:
        entries = entries * shard_levels(stream_key, extent, cuts, -0.22, 0.18)
    return jnp.clip(spiked(entries, jax.random.fold_in(stream_key, 3), *heavy), -limit, limit).astype(held_as)


def setup_inputs(seed: int = 0) -> dict:
    arg_keys = jax.random.split(jax.random.key(seed), 9)
    cells_next = noise(arg_keys[0], (CELLS, D), 1.0, 6.0, ((0, 64), (1, 4)))
    node_embed = noise(arg_keys[1], (NODES, D), 1.0, 6.0, ((0, 64), (1, 4)))
    enc_mix = noise(arg_keys[2], (D, D), D ** -0.5, 0.1875, ((1, 4),))
    out_cotangent = heavy_noise(arg_keys[3], (CELLS, D), 1.0, 16.0, ((0, 64), (1, 4)), (0, 1, 64, 4.0))
    decoded_saved = noise(arg_keys[4], (CELLS, D), 1.0, 6.0, ((0, 64), (1, 4)))
    dec_proj = noise(arg_keys[5], (D, D), D ** -0.5, 0.1875, ((1, 4),))
    tile_source = draw_tile_source(jax.random.fold_in(arg_keys[8], 71), 0)
    tile_codes = plant(jax.random.randint(arg_keys[7], (NODE_BLOCKS, K, BLK, BLK), 0, 65536), jax.random.fold_in(arg_keys[7], 1), 0, 65535).astype(jnp.int32)
    return {"cells_next": cells_next, "node_embed": node_embed, "enc_mix": enc_mix, "out_cotangent": out_cotangent, "decoded_saved": decoded_saved, "dec_proj": dec_proj, "tile_source": tile_source, "tile_codes": tile_codes}


def split_codes(code_words):
    low_codes = (code_words % 256 - 128).astype(jnp.bfloat16)
    high_codes = (code_words // 256 - 128).astype(jnp.bfloat16)
    return low_codes, high_codes


def reference(cells_next, node_embed, enc_mix, out_cotangent, decoded_saved, dec_proj, tile_source, tile_codes):
    tile_scale = (3.0 / (K * BLK)) ** 0.5 / 128.0
    channels = cells_next.shape[1]
    cotangent_wide = out_cotangent.astype(jnp.float32)
    cell_grad = jnp.dot(cotangent_wide, dec_proj.astype(jnp.float32), preferred_element_type=jnp.float32).astype(jnp.bfloat16)
    cell_blocks = cells_next.reshape(-1, BLK, channels)
    grad_blocks = cell_grad.reshape(-1, BLK, channels)

    def per_block(inputs):
        sources, code_words = inputs
        enc_tile, dec_tile = split_codes(code_words)
        gathered = cell_blocks[sources].astype(jnp.float32)
        aggregate = jnp.einsum("kab,kbd->ad", enc_tile.astype(jnp.float32), gathered) * tile_scale
        grad_rows = grad_blocks[sources].astype(jnp.float32)
        node_part = jnp.einsum("kab,kbd->ad", dec_tile.astype(jnp.float32), grad_rows) * tile_scale
        return aggregate.astype(jnp.bfloat16), node_part.astype(jnp.bfloat16)

    agg_blocks, node_blocks = lax.map(per_block, (tile_source, tile_codes))
    aggregate = agg_blocks.reshape(-1, channels)
    mixed_rows = jnp.dot(aggregate, enc_mix, preferred_element_type=jnp.float32)
    hidden_nodes = (node_embed.astype(jnp.float32) + jax.nn.silu(mixed_rows)).astype(jnp.bfloat16)
    node_grad = node_blocks.reshape(-1, channels)
    w_dec_grad = jnp.dot(cotangent_wide.T, decoded_saved.astype(jnp.float32), preferred_element_type=jnp.float32) * (CELLS ** -0.5)
    return hidden_nodes, node_grad, w_dec_grad
```

```python
import functools

import jax
import jax.numpy as jnp
from jax import lax
from jax.experimental import pallas as pl
from jax.experimental.pallas import tpu as pltpu
from jax.sharding import PartitionSpec as P

BLK = 128
K = 16
R = 3
CB_DEV = 16
NB_DEV = 2
CAP = 8
CHAN = 4
TILES = NB_DEV * K
PAIR_BLOCKS = 2 * CB_DEV
SIDE = 2 * CAP


def permute(x, move, bands):
    pairs = []
    for band in range(bands):
        for chan in range(CHAN):
            to_band, to_chan = move(band, chan)
            if 0 <= to_band < bands:
                pairs.append((band * CHAN + chan, to_band * CHAN + to_chan))
    return lax.ppermute(x, ("band", "chan"), pairs)


def far_step(band):
    return 2 if band % 2 == 0 else -2


def slot_table(tile_source, readers, offsets):
    bands = tile_source.shape[0] // NB_DEV
    rows = tile_source.reshape(bands, TILES)[jnp.clip(readers, 0, bands - 1)]
    hit = (rows // PAIR_BLOCKS - (readers // 2)[:, None]) == offsets[:, None]
    earlier = jnp.tril(jnp.ones((TILES, TILES), jnp.int32), -1)
    rank = jnp.sum(hit.astype(jnp.int32)[:, None, :] * earlier[None], axis=2)
    code = (jnp.arange(TILES, dtype=jnp.int32) * PAIR_BLOCKS)[None] + rows % PAIR_BLOCKS + 1
    chosen = hit[:, None, :] & (rank[:, None, :] == jnp.arange(SIDE, dtype=jnp.int32)[None, :, None])
    packed = jnp.sum(jnp.where(chosen, code[:, None, :], 0), axis=2) - 1
    tile = jnp.where(packed < 0, -1, packed // PAIR_BLOCKS)
    block = jnp.where(packed < 0, 0, packed % PAIR_BLOCKS)
    return tile, block


def products_kernel(groups, n_codes, *refs):
    meta = refs[0]
    codes = refs[1 : 1 + n_codes]
    cells_own, cells_sib, cot_own, cot_sib = refs[1 + n_codes : 5 + n_codes]
    outs = refs[5 + n_codes : 5 + n_codes + len(groups)]
    code_buf, cell_buf, cot_buf, total, sems = refs[5 + n_codes + len(groups) :]

    for parts in groups:
        for operand, first, count in parts:
            source = codes[operand]

            def begin(i, carry, first=first, source=source):
                slot = first + i
                pltpu.make_async_copy(source.at[meta[3, slot]], code_buf.at[slot], sems.at[0, slot]).start()
                local = meta[2, slot]

                @pl.when(meta[1, slot] == 1)
                def _():
                    pltpu.make_async_copy(cells_own.at[local], cell_buf.at[slot], sems.at[1, slot]).start()
                    pltpu.make_async_copy(cot_own.at[local], cot_buf.at[slot], sems.at[2, slot]).start()

                @pl.when(meta[1, slot] != 1)
                def _():
                    pltpu.make_async_copy(cells_sib.at[local], cell_buf.at[slot], sems.at[1, slot]).start()
                    pltpu.make_async_copy(cot_sib.at[local], cot_buf.at[slot], sems.at[2, slot]).start()

                return carry

            lax.fori_loop(0, count, begin, 0)

    for out, parts in zip(outs, groups):
        total[...] = jnp.zeros_like(total)
        first = parts[0][1]
        slots = sum(count for _, _, count in parts)

        def step(i, carry, first=first):
            for inner in range(4):
                slot = first + i * 4 + inner
                pltpu.make_async_copy(codes[0].at[0], code_buf.at[slot], sems.at[0, slot]).wait()
                pltpu.make_async_copy(cells_own.at[0], cell_buf.at[slot], sems.at[1, slot]).wait()
                pltpu.make_async_copy(cot_own.at[0], cot_buf.at[slot], sems.at[2, slot]).wait()
                words = code_buf[slot]
                enc = ((words & 255) - 128).astype(jnp.float32).astype(jnp.bfloat16)
                dec = ((words >> 8) - 128).astype(jnp.float32).astype(jnp.bfloat16)
                node = meta[0, slot]
                total[0, node] += jnp.dot(enc, cell_buf[slot], preferred_element_type=jnp.float32)
                total[1, node] += jnp.dot(dec, cot_buf[slot], preferred_element_type=jnp.float32)
            return carry

        lax.fori_loop(0, slots // 4, step, 0)
        for kind in range(2):
            for node in range(NB_DEV):
                out[kind, node] = total[kind, node].astype(out.dtype)


def tile_products(meta, codes, blocks, groups, dtypes):
    slots = meta.shape[1]
    channels = blocks[0].shape[-1]
    flops = slots * 4 * BLK * BLK * channels
    moved = slots * (BLK * BLK * 4 + 2 * BLK * channels * 2)
    return pl.pallas_call(
        functools.partial(products_kernel, groups, len(codes)),
        out_shape=[jax.ShapeDtypeStruct((2, NB_DEV, BLK, channels), dtype) for dtype in dtypes],
        in_specs=[pl.BlockSpec(memory_space=pltpu.SMEM)]
        + [pl.BlockSpec(memory_space=pl.ANY)] * (len(codes) + 4),
        out_specs=[pl.BlockSpec(memory_space=pltpu.VMEM)] * len(dtypes),
        scratch_shapes=[
            pltpu.VMEM((slots, BLK, BLK), jnp.int32),
            pltpu.VMEM((slots, BLK, channels), jnp.bfloat16),
            pltpu.VMEM((slots, BLK, channels), jnp.bfloat16),
            pltpu.VMEM((2, NB_DEV + 1, BLK, channels), jnp.float32),
            pltpu.SemaphoreType.DMA((3, slots)),
        ],
        cost_estimate=pl.CostEstimate(flops=flops, bytes_accessed=moved, transcendentals=0),
        name="tile_products",
    )(meta, *codes, *blocks)


def project_kernel(chan_ref, p0, p1, p2, p3, enc_mix, dec_proj, node_embed, hidden, node_grad):
    chan = chan_ref[0]
    mixed = None
    for back, piece in enumerate((p0, p1, p2, p3)):
        rows = pl.ds(pl.multiple_of(((chan + CHAN - back) % CHAN) * 256, 256), 256)
        left = jnp.dot(piece[0], enc_mix[rows, :], preferred_element_type=jnp.float32)
        right = jnp.dot(piece[1], dec_proj[rows, :], preferred_element_type=jnp.float32)
        mixed, grad = (left, right) if mixed is None else (mixed + left, grad + right)
    hidden[...] = (node_embed[...].astype(jnp.float32) + mixed / (1.0 + jnp.exp(-mixed))).astype(hidden.dtype)
    node_grad[...] = grad.astype(node_grad.dtype)


def project(chan, pieces, enc_mix, dec_proj, node_embed):
    rows, channels = node_embed.shape
    vmem = pl.BlockSpec(memory_space=pltpu.VMEM)
    return pl.pallas_call(
        project_kernel,
        out_shape=[jax.ShapeDtypeStruct((rows, channels), jnp.bfloat16)] * 2,
        in_specs=[pl.BlockSpec(memory_space=pltpu.SMEM)] + [vmem] * 7,
        out_specs=[vmem] * 2,
        cost_estimate=pl.CostEstimate(
            flops=4 * rows * CHAN * channels * channels,
            bytes_accessed=4 * CHAN * rows * channels * 4,
            transcendentals=rows * channels,
        ),
        name="project",
    )(chan.reshape(1), *pieces, enc_mix, dec_proj, node_embed)


def shards(
    cells_next, node_embed, enc_mix, out_cotangent, decoded_saved, dec_proj, tile_source, tile_codes
):
    bands = lax.axis_size("band")
    band = lax.axis_index("band")
    chan = lax.axis_index("chan")
    core = band % 2
    tile_scale = (3.0 / (K * BLK)) ** 0.5 / 128.0
    channels = cells_next.shape[1]
    go = functools.partial(permute, bands=bands)
    codes = tile_codes.reshape(TILES, BLK, BLK)
    cells = cells_next.reshape(CB_DEV, BLK, channels)
    cotangent = out_cotangent.reshape(CB_DEV, BLK, channels)

    far = jnp.where(core == 0, 2, -2)
    readers = jnp.stack([band, band, band, band, band + 2, band - 2, band + 2 * far])
    offsets = jnp.stack([-1 + 0 * far, 1 + 0 * far, -far, 0 * far, -1 + 0 * far, 1 + 0 * far, -far])
    tile, block = slot_table(tile_source, readers, offsets)

    def quarter_for(row):
        wanted = lax.dynamic_slice_in_dim(row, (CHAN - 1 - chan) * (SIDE // CHAN), SIDE // CHAN, 0)
        return codes[jnp.maximum(wanted, 0)]

    to_below = go(quarter_for(tile[0]), lambda b, c: (b - 2, CHAN - 1 - c))
    to_above = go(quarter_for(tile[1]), lambda b, c: (b + 2, CHAN - 1 - c))
    to_far = go(codes[jnp.maximum(tile[2, :CAP], 0)], lambda b, c: (b - 2 * far_step(b), c))
    cells_sib = go(cells, lambda b, c: (b ^ 1, c))
    cotangent_sib = go(cotangent, lambda b, c: (b ^ 1, c))

    def over_chan(x):
        return [x] + [go(x, lambda b, c, by=by: (b, (c + by) % CHAN)) for by in range(1, CHAN)]

    codes_up = over_chan(to_below)
    codes_down = over_chan(to_above)

    cot_pair = go(out_cotangent, lambda b, c: (b, c ^ 1))
    dec_pair = go(decoded_saved, lambda b, c: (b, c ^ 2))

    def meta_of(row, slots, index):
        node = jnp.where(tile[row] < 0, NB_DEV, tile[row] // K)
        own = (block[row] // CB_DEV == core).astype(jnp.int32)
        return jnp.stack([node, own, block[row] % CB_DEV, index])[:, :slots]

    def pieces_meta(row):
        order = ((chan + CHAN - jnp.arange(CHAN)) % CHAN)[:, None] * (SIDE // CHAN) + jnp.arange(SIDE // CHAN)[None]
        index = jnp.tile(jnp.arange(SIDE // CHAN, dtype=jnp.int32), CHAN)
        meta = meta_of(row, SIDE, index)[:, order.reshape(-1)]
        return meta.at[3].set(index)

    blocks = (cells, cells_sib, cotangent, cotangent_sib)
    piece_group = [[(i, i * (SIDE // CHAN), SIDE // CHAN) for i in range(CHAN)]]
    near_meta = jnp.concatenate(
        [meta_of(6, CAP, jnp.arange(SIDE, dtype=jnp.int32)), meta_of(3, SIDE, jnp.maximum(tile[3], 0))], axis=1
    )
    far_part, own_part = tile_products(
        near_meta, [to_far, codes], blocks, [[(0, 0, CAP)], [(1, CAP, SIDE)]], [jnp.bfloat16, jnp.float32]
    )
    (up_part,) = tile_products(pieces_meta(4), codes_up, blocks, piece_group, [jnp.bfloat16])
    (down_part,) = tile_products(pieces_meta(5), codes_down, blocks, piece_group, [jnp.bfloat16])

    got_below = go(up_part, lambda b, c: (b + 2, c))
    got_above = go(down_part, lambda b, c: (b - 2, c))
    got_far = go(far_part, lambda b, c: (b + 2 * far_step(b), c))
    summed = (
        own_part
        + got_below.astype(jnp.float32)
        + got_above.astype(jnp.float32)
        + got_far.astype(jnp.float32)
    )
    aggregates = (summed * tile_scale).astype(jnp.bfloat16).reshape(2, NB_DEV * BLK, channels)
    hidden_nodes, node_grad = project(chan, over_chan(aggregates), enc_mix, dec_proj, node_embed)

    def outer(left, right):
        return lax.dot_general(
            left, right, (((0,), (0,)), ((), ())), preferred_element_type=jnp.float32
        ).astype(jnp.bfloat16)

    grid = jnp.stack(
        [
            outer(out_cotangent, decoded_saved),
            outer(cot_pair, decoded_saved),
            outer(out_cotangent, dec_pair),
            outer(cot_pair, dec_pair),
        ]
    )
    shares = grid[jnp.arange(CHAN) ^ chan].reshape(bands, -1, channels)
    shares = lax.all_to_all(shares, "band", 0, 0, tiled=True)
    share = jnp.sum(shares.astype(jnp.float32), axis=0)
    per_x = bands // CHAN

    def home(b, c):
        x, rest = b // per_x, b % per_x
        return (2 * (c // 2) + x % 2) * per_x + rest, c % 2 + 2 * (x // 2)

    cells_total = cells_next.shape[0] * bands
    w_dec_grad = go(share, home) * cells_total ** (-0.5)
    return (hidden_nodes, node_grad, w_dec_grad)


def solution(mesh):
    in_specs = (
        P("band", "chan"),
        P("band", "chan"),
        P(None, "chan"),
        P("band", "chan"),
        P("band", "chan"),
        P(None, "chan"),
        P(),
        P("band", None, None, None),
    )
    out_specs = (P("band", "chan"), P("band", "chan"), P("band", "chan"))
    return jax.shard_map(shards, mesh=mesh, in_specs=in_specs, out_specs=out_specs, check_vma=False)
```

```python
import functools

import jax
import jax.numpy as jnp
from jax import lax
from jax.experimental import pallas as pl
from jax.experimental.pallas import tpu as pltpu
from jax.sharding import PartitionSpec as P


BLK = 128
K = 16
CB_DEV = 16
NB_DEV = 2
CAP = 8
CHAN = 4
TILES = NB_DEV * K
PAIR_BLOCKS = 2 * CB_DEV
SIDE = 2 * CAP


def permute(x, move, bands):
    pairs = []
    for band in range(bands):
        for chan in range(CHAN):
            to_band, to_chan = move(band, chan)
            if 0 <= to_band < bands:
                pairs.append((band * CHAN + chan, to_band * CHAN + to_chan))
    return lax.ppermute(x, ("band", "chan"), pairs)


def far_step(band):
    return 2 if band % 2 == 0 else -2


def slot_table(tile_source, readers, offsets):
    bands = tile_source.shape[0] // NB_DEV
    rows = tile_source.reshape(bands, TILES)[jnp.clip(readers, 0, bands - 1)]
    hit = (rows // PAIR_BLOCKS - (readers // 2)[:, None]) == offsets[:, None]
    earlier = jnp.tril(jnp.ones((TILES, TILES), jnp.int32), -1)
    rank = jnp.sum(hit.astype(jnp.int32)[:, None, :] * earlier[None], axis=2)
    code = (jnp.arange(TILES, dtype=jnp.int32) * PAIR_BLOCKS)[None] + rows % PAIR_BLOCKS + 1
    chosen = hit[:, None, :] & (rank[:, None, :] == jnp.arange(SIDE, dtype=jnp.int32)[None, :, None])
    packed = jnp.sum(jnp.where(chosen, code[:, None, :], 0), axis=2) - 1
    tile = jnp.where(packed < 0, -1, packed // PAIR_BLOCKS)
    block = jnp.where(packed < 0, 0, packed % PAIR_BLOCKS)
    return tile, block


def pick_kernel(pick, codes, *refs):
    outs, sems = refs[:-1], refs[-1]
    places = [(out, i) for out in outs for i in range(out.shape[0])]
    copies = [
        pltpu.make_async_copy(codes.at[pick[slot]], out.at[i], sems.at[slot])
        for slot, (out, i) in enumerate(places)
    ]
    for copy in copies:
        copy.start()
    for copy in copies:
        copy.wait()


def pick_tiles(pick, codes, counts):
    return pl.pallas_call(
        pick_kernel,
        out_shape=[jax.ShapeDtypeStruct((count, BLK, BLK), codes.dtype) for count in counts],
        in_specs=[pl.BlockSpec(memory_space=pltpu.SMEM), pl.BlockSpec(memory_space=pl.ANY)],
        out_specs=[pl.BlockSpec(memory_space=pltpu.VMEM)] * len(counts),
        scratch_shapes=[pltpu.SemaphoreType.DMA((sum(counts),))],
        cost_estimate=pl.CostEstimate(flops=10**8, bytes_accessed=2 * sum(counts) * BLK * BLK * 4, transcendentals=0),
        name="pick_tiles",
    )(pick, codes)


def products_kernel(groups, n_codes, *refs):
    meta = refs[0]
    codes = refs[1 : 1 + n_codes]
    cells_own, cells_sib, cot_own, cot_sib = refs[1 + n_codes : 5 + n_codes]
    outs = refs[5 + n_codes : 5 + n_codes + len(groups)]
    code_buf, cell_buf, cot_buf, total, sems = refs[5 + n_codes + len(groups) :]
    for parts in groups:
        for operand, first, count in parts:
            source = codes[operand]

            def begin(i, carry, first=first, source=source):
                slot = first + i
                pltpu.make_async_copy(source.at[meta[3, slot]], code_buf.at[slot], sems.at[0, slot]).start()
                local = meta[2, slot]

                @pl.when(meta[1, slot] == 1)
                def _():
                    pltpu.make_async_copy(cells_own.at[local], cell_buf.at[slot], sems.at[1, slot]).start()
                    pltpu.make_async_copy(cot_own.at[local], cot_buf.at[slot], sems.at[2, slot]).start()

                @pl.when(meta[1, slot] != 1)
                def _():
                    pltpu.make_async_copy(cells_sib.at[local], cell_buf.at[slot], sems.at[1, slot]).start()
                    pltpu.make_async_copy(cot_sib.at[local], cot_buf.at[slot], sems.at[2, slot]).start()

                return carry

            lax.fori_loop(0, count, begin, 0)

    for out, parts in zip(outs, groups):
        total[...] = jnp.zeros_like(total)
        first = parts[0][1]
        slots = sum(count for _, _, count in parts)

        def step(i, carry, first=first):
            enc_rows, dec_rows = [[], []], [[], []]
            base = first + i * 4
            for inner in range(4):
                slot = base + inner
                pltpu.make_async_copy(codes[0].at[0], code_buf.at[slot], sems.at[0, slot]).wait()
                pltpu.make_async_copy(cells_own.at[0], cell_buf.at[slot], sems.at[1, slot]).wait()
                pltpu.make_async_copy(cot_own.at[0], cot_buf.at[slot], sems.at[2, slot]).wait()
                words = code_buf[slot]
                enc = ((words & 255) - 128).astype(jnp.float32)
                dec = ((words >> 8) - 128).astype(jnp.float32)
                for node in range(NB_DEV):
                    keep = (meta[0, slot] == node).astype(jnp.float32)
                    enc_rows[node].append((enc * keep).astype(jnp.bfloat16))
                    dec_rows[node].append((dec * keep).astype(jnp.bfloat16))
            wide = [
                jnp.concatenate([jnp.concatenate(line, axis=1) for line in both], axis=0)
                for both in (enc_rows, dec_rows)
            ]
            cells = cell_buf[pl.ds(base, 4)].reshape(4 * BLK, -1)
            cots = cot_buf[pl.ds(base, 4)].reshape(4 * BLK, -1)
            total[0] += jnp.dot(wide[0], cells, preferred_element_type=jnp.float32)
            total[1] += jnp.dot(wide[1], cots, preferred_element_type=jnp.float32)
            return carry

        lax.fori_loop(0, slots // 4, step, 0)
        out[...] = total[...].astype(out.dtype)


def tile_products(meta, codes, blocks, groups, dtypes):
    slots = meta.shape[1]
    channels = blocks[0].shape[-1]
    flops = slots * 4 * BLK * BLK * channels
    moved = slots * (BLK * BLK * 4 + 2 * BLK * channels * 2)
    return pl.pallas_call(
        functools.partial(products_kernel, groups, len(codes)),
        out_shape=[jax.ShapeDtypeStruct((2, NB_DEV * BLK, channels), dtype) for dtype in dtypes],
        in_specs=[pl.BlockSpec(memory_space=pltpu.SMEM)]
        + [pl.BlockSpec(memory_space=pl.ANY)] * (len(codes) + 4),
        out_specs=[pl.BlockSpec(memory_space=pltpu.VMEM)] * len(dtypes),
        scratch_shapes=[
            pltpu.VMEM((slots, BLK, BLK), jnp.int32),
            pltpu.VMEM((slots, BLK, channels), jnp.bfloat16),
            pltpu.VMEM((slots, BLK, channels), jnp.bfloat16),
            pltpu.VMEM((2, NB_DEV * BLK, channels), jnp.float32),
            pltpu.SemaphoreType.DMA((3, slots)),
        ],
        cost_estimate=pl.CostEstimate(flops=flops, bytes_accessed=moved, transcendentals=0),
        name="tile_products",
    )(meta, *codes, *blocks)


def project_kernel(chan_ref, p0, p1, p2, p3, enc_mix, dec_proj, node_embed, hidden, node_grad):
    chan = chan_ref[0]
    mixed = None
    for back, piece in enumerate((p0, p1, p2, p3)):
        rows = pl.ds(pl.multiple_of(((chan + CHAN - back) % CHAN) * 256, 256), 256)
        left = jnp.dot(piece[0], enc_mix[rows, :], preferred_element_type=jnp.float32)
        right = jnp.dot(piece[1], dec_proj[rows, :], preferred_element_type=jnp.float32)
        mixed, grad = (left, right) if mixed is None else (mixed + left, grad + right)
    hidden[...] = (node_embed[...].astype(jnp.float32) + mixed / (1.0 + jnp.exp(-mixed))).astype(hidden.dtype)
    node_grad[...] = grad.astype(node_grad.dtype)


def project(chan, pieces, enc_mix, dec_proj, node_embed):
    rows, channels = node_embed.shape
    vmem = pl.BlockSpec(memory_space=pltpu.VMEM)
    return pl.pallas_call(
        project_kernel,
        out_shape=[jax.ShapeDtypeStruct((rows, channels), jnp.bfloat16)] * 2,
        in_specs=[pl.BlockSpec(memory_space=pltpu.SMEM)] + [vmem] * 7,
        out_specs=[vmem] * 2,
        cost_estimate=pl.CostEstimate(
            flops=4 * rows * CHAN * channels * channels,
            bytes_accessed=4 * CHAN * rows * channels * 4,
            transcendentals=rows * channels,
        ),
        name="project",
    )(chan.reshape(1), *pieces, enc_mix, dec_proj, node_embed)


def near_step(band):
    return 1 - 2 * (band // 2 % 2)


def one_device(
    cells_next, node_embed, enc_mix, out_cotangent, decoded_saved, dec_proj, tile_source, tile_codes
):
    bands = lax.axis_size("band")
    band = lax.axis_index("band")
    chan = lax.axis_index("chan")
    core = band % 2
    tile_scale = (3.0 / (K * BLK)) ** 0.5 / 128.0
    channels = cells_next.shape[1]
    go = functools.partial(permute, bands=bands)
    codes = tile_codes.reshape(TILES, BLK, BLK)
    cells = cells_next.reshape(CB_DEV, BLK, channels)
    cotangent = out_cotangent.reshape(CB_DEV, BLK, channels)
    quarter = SIDE // CHAN

    cells_sib = go(cells, lambda b, c: (b ^ 1, c))
    cotangent_sib = go(cotangent, lambda b, c: (b ^ 1, c))

    near = near_step(band)
    far = far_step_traced(core)
    readers = band + jnp.array([0, 0, 0, 0, 2, -2, 0], jnp.int32) * near + jnp.array([0] * 6 + [2], jnp.int32) * far
    offsets = (
        jnp.array([1, -1, 0, 0, -1, 1, 0], jnp.int32) * near + jnp.array([0, 0, -1, 0, 0, 0, -1], jnp.int32) * far
    )
    tile, block = slot_table(tile_source, readers, offsets)

    wanted = lax.dynamic_slice_in_dim(tile[:2], (CHAN - 1 - chan) * quarter, quarter, 1)
    pick = jnp.maximum(jnp.concatenate([wanted.reshape(-1), tile[2, :CAP]]), 0)
    keep_codes, give_codes, far_codes = pick_tiles(pick, codes, (quarter, quarter, CAP))
    give_codes = go(give_codes, lambda b, c: (b - 2 * near_step(b), CHAN - 1 - c))
    keep_codes = go(keep_codes, lambda b, c: (b ^ 2, CHAN - 1 - c))
    far_codes = go(far_codes, lambda b, c: (b - 2 * far_step(b), c))

    def over_chan(x):
        return [x] + [go(x, lambda b, c, by=by: (b, (c + by) % CHAN)) for by in range(1, CHAN)]

    give_codes = over_chan(give_codes)
    keep_codes = over_chan(keep_codes)

    cot_pair = go(out_cotangent, lambda b, c: (b, c ^ 1))
    dec_pair = go(decoded_saved, lambda b, c: (b, c ^ 2))

    def meta_of(row, index):
        node = jnp.where(tile[row] < 0, NB_DEV, tile[row] // K)
        own = (block[row] // CB_DEV == core).astype(jnp.int32)
        return jnp.stack([node, own, block[row] % CB_DEV, index])

    def pieces_meta(row):
        meta = meta_of(row, jnp.arange(SIDE, dtype=jnp.int32) % quarter)
        double = jnp.concatenate([meta, meta], axis=1)
        parts = [
            lax.dynamic_slice_in_dim(double, (chan + CHAN - i) * quarter, quarter, 1) for i in range(CHAN)
        ]
        return jnp.concatenate(parts, axis=1)

    blocks = (cells, cells_sib, cotangent, cotangent_sib)
    piece_group = [[(i, i * quarter, quarter) for i in range(CHAN)]]
    near_meta = jnp.concatenate(
        [meta_of(6, jnp.arange(SIDE, dtype=jnp.int32))[:, :CAP], meta_of(3, jnp.maximum(tile[3], 0))], axis=1
    )
    far_part, own_part = tile_products(
        near_meta, [far_codes, codes], blocks, [[(0, 0, CAP)], [(1, CAP, SIDE)]], [jnp.bfloat16, jnp.float32]
    )
    got_far = go(far_part, lambda b, c: (b + 2 * far_step(b), c))
    (give_part,) = tile_products(pieces_meta(5), give_codes, blocks, piece_group, [jnp.bfloat16])
    got_give = go(give_part, lambda b, c: (b - 4 * near_step(b), c))
    (keep_part,) = tile_products(pieces_meta(4), keep_codes, blocks, piece_group, [jnp.float32])
    crossing = (keep_part + got_give.astype(jnp.float32)).astype(jnp.bfloat16)
    got_keep = go(crossing, lambda b, c: (b ^ 2, c))
    summed = own_part + got_keep.astype(jnp.float32) + got_far.astype(jnp.float32)
    aggregates = (summed * tile_scale).astype(jnp.bfloat16)
    pieces = over_chan(aggregates)
    hidden_nodes, node_grad = project(chan, pieces, enc_mix, dec_proj, node_embed)

    w_dec_grad = projection_gradient(go, out_cotangent, decoded_saved, cot_pair, dec_pair, bands)
    return (hidden_nodes, node_grad, w_dec_grad)


def far_step_traced(core):
    return 2 - 4 * core


def projection_gradient(go, cot, dec, cot_pair, dec_pair, bands):
    band, chan = lax.axis_index("band"), lax.axis_index("chan")
    along = bands // 16
    x, y, zh, core = band // (4 * along), band // along % 4, band // 2 % 2, band % 2
    channels = cot.shape[1]
    cells_total = cot.shape[0] * bands
    rows = channels // 16

    def outer(left, right):
        return lax.dot_general(left, right, (((0,), (0,)), ((), ())), preferred_element_type=jnp.float32)

    whole = jnp.stack([outer(cot, dec), outer(cot_pair, dec), outer(cot, dec_pair), outer(cot_pair, dec_pair)])
    halves = whole.reshape(4, 8, 2, rows, channels)
    own = lax.dynamic_index_in_dim(halves, core, 2, keepdims=False)
    other = lax.dynamic_index_in_dim(halves, 1 - core, 2, keepdims=False).astype(jnp.bfloat16)
    own = own + go(other, lambda b, c: (b ^ 1, c)).astype(jnp.float32)

    def take(i):
        return lax.dynamic_index_in_dim(own, i, 0, keepdims=False)

    share = take(x ^ chan)
    for by in range(1, 4):
        sent = take(((x + by) % 4) ^ chan).astype(jnp.bfloat16)
        share = share + go(sent, lambda b, c: ((b + by * 4 * along) % bands, c)).astype(jnp.float32)

    own = share.reshape(4, 2, rows, channels)
    share = take(y)
    for by in range(1, 4):
        sent = take((y + by) % 4)
        share = share + go(sent, lambda b, c: (b // 16 * 16 + (b % 16 + by * 4) % 16, c))

    def home(b, c):
        at_x, rest = b // 16, b % 16
        return (2 * (c // 2) + at_x % 2) * 16 + rest, c % 2 + 2 * (at_x // 2)

    def home_across(b, c):
        return home(b ^ 2, c)

    own = share
    return (go(take(zh), home) + go(take(1 - zh), home_across)) * cells_total ** (-0.5)


def solution(mesh):
    in_specs = (
        P("band", "chan"),
        P("band", "chan"),
        P(None, "chan"),
        P("band", "chan"),
        P("band", "chan"),
        P(None, "chan"),
        P(),
        P("band", None, None, None),
    )
    out_specs = (P("band", "chan"), P("band", "chan"), P("band", "chan"))
    return jax.shard_map(one_device, mesh=mesh, in_specs=in_specs, out_specs=out_specs, check_vma=False)
```

```python
import functools

import jax
import jax.numpy as jnp
from jax import lax
from jax.experimental import pallas as pl
from jax.experimental.pallas import tpu as pltpu
from jax.sharding import PartitionSpec as P


BLK = 128
K = 16
CB_DEV = 16
NB_DEV = 2
CAP = 8
CHAN = 4
TILES = NB_DEV * K
PAIR_BLOCKS = 2 * CB_DEV
SIDE = 2 * CAP


def permute(x, move, bands):
    pairs = []
    for band in range(bands):
        for chan in range(CHAN):
            to_band, to_chan = move(band, chan)
            if 0 <= to_band < bands:
                pairs.append((band * CHAN + chan, to_band * CHAN + to_chan))
    return lax.ppermute(x, ("band", "chan"), pairs)


def far_step(band):
    return 2 if band % 2 == 0 else -2


def slot_table(tile_source, readers, offsets):
    bands = tile_source.shape[0] // NB_DEV
    rows = tile_source.reshape(bands, TILES)[jnp.clip(readers, 0, bands - 1)]
    hit = (rows // PAIR_BLOCKS - (readers // 2)[:, None]) == offsets[:, None]
    earlier = jnp.tril(jnp.ones((TILES, TILES), jnp.int32), -1)
    rank = jnp.sum(hit.astype(jnp.int32)[:, None, :] * earlier[None], axis=2)
    code = (jnp.arange(TILES, dtype=jnp.int32) * PAIR_BLOCKS)[None] + rows % PAIR_BLOCKS + 1
    chosen = hit[:, None, :] & (rank[:, None, :] == jnp.arange(SIDE, dtype=jnp.int32)[None, :, None])
    packed = jnp.sum(jnp.where(chosen, code[:, None, :], 0), axis=2) - 1
    tile = jnp.where(packed < 0, -1, packed // PAIR_BLOCKS)
    block = jnp.where(packed < 0, 0, packed % PAIR_BLOCKS)
    return tile, block


def pick_kernel(pick, codes, *refs):
    outs, sems = refs[:-1], refs[-1]
    places = [(out, i) for out in outs for i in range(out.shape[0])]
    copies = [
        pltpu.make_async_copy(codes.at[pick[slot]], out.at[i], sems.at[slot])
        for slot, (out, i) in enumerate(places)
    ]
    for copy in copies:
        copy.start()
    for copy in copies:
        copy.wait()


def pick_tiles(pick, codes, counts):
    return pl.pallas_call(
        pick_kernel,
        out_shape=[jax.ShapeDtypeStruct((count, BLK, BLK), codes.dtype) for count in counts],
        in_specs=[pl.BlockSpec(memory_space=pltpu.SMEM), pl.BlockSpec(memory_space=pl.ANY)],
        out_specs=[pl.BlockSpec(memory_space=pltpu.VMEM)] * len(counts),
        scratch_shapes=[pltpu.SemaphoreType.DMA((sum(counts),))],
        cost_estimate=pl.CostEstimate(flops=10**8, bytes_accessed=2 * sum(counts) * BLK * BLK * 4, transcendentals=0),
        name="pick_tiles",
    )(pick, codes)


def products_kernel(groups, n_codes, *refs):
    meta = refs[0]
    codes = refs[1 : 1 + n_codes]
    cells_own, cells_sib, cot_own, cot_sib = refs[1 + n_codes : 5 + n_codes]
    outs = refs[5 + n_codes : 5 + n_codes + len(groups)]
    code_buf, cell_buf, cot_buf, total, sems = refs[5 + n_codes + len(groups) :]
    for parts in groups:
        for operand, first, count in parts:
            source = codes[operand]

            def begin(i, carry, first=first, source=source):
                slot = first + i
                pltpu.make_async_copy(source.at[meta[3, slot]], code_buf.at[slot], sems.at[0, slot]).start()
                local = meta[2, slot]

                @pl.when(meta[1, slot] == 1)
                def _():
                    pltpu.make_async_copy(cells_own.at[local], cell_buf.at[slot], sems.at[1, slot]).start()
                    pltpu.make_async_copy(cot_own.at[local], cot_buf.at[slot], sems.at[2, slot]).start()

                @pl.when(meta[1, slot] != 1)
                def _():
                    pltpu.make_async_copy(cells_sib.at[local], cell_buf.at[slot], sems.at[1, slot]).start()
                    pltpu.make_async_copy(cot_sib.at[local], cot_buf.at[slot], sems.at[2, slot]).start()

                return carry

            lax.fori_loop(0, count, begin, 0)

    for out, parts in zip(outs, groups):
        total[...] = jnp.zeros_like(total)
        first = parts[0][1]
        slots = sum(count for _, _, count in parts)

        def step(i, carry, first=first):
            enc_rows, dec_rows = [[], []], [[], []]
            base = first + i * 4
            for inner in range(4):
                slot = base + inner
                pltpu.make_async_copy(codes[0].at[0], code_buf.at[slot], sems.at[0, slot]).wait()
                pltpu.make_async_copy(cells_own.at[0], cell_buf.at[slot], sems.at[1, slot]).wait()
                pltpu.make_async_copy(cot_own.at[0], cot_buf.at[slot], sems.at[2, slot]).wait()
                words = code_buf[slot]
                enc = ((words & 255) - 128).astype(jnp.float32)
                dec = ((words >> 8) - 128).astype(jnp.float32)
                for node in range(NB_DEV):
                    keep = (meta[0, slot] == node).astype(jnp.float32)
                    enc_rows[node].append((enc * keep).astype(jnp.bfloat16))
                    dec_rows[node].append((dec * keep).astype(jnp.bfloat16))
            wide = [
                jnp.concatenate([jnp.concatenate(line, axis=1) for line in both], axis=0)
                for both in (enc_rows, dec_rows)
            ]
            cells = cell_buf[pl.ds(base, 4)].reshape(4 * BLK, -1)
            cots = cot_buf[pl.ds(base, 4)].reshape(4 * BLK, -1)
            total[0] += jnp.dot(wide[0], cells, preferred_element_type=jnp.float32)
            total[1] += jnp.dot(wide[1], cots, preferred_element_type=jnp.float32)
            return carry

        lax.fori_loop(0, slots // 4, step, 0)
        out[...] = total[...].astype(out.dtype)


def tile_products(meta, codes, blocks, groups, dtypes):
    slots = meta.shape[1]
    channels = blocks[0].shape[-1]
    flops = slots * 4 * BLK * BLK * channels
    moved = slots * (BLK * BLK * 4 + 2 * BLK * channels * 2)
    return pl.pallas_call(
        functools.partial(products_kernel, groups, len(codes)),
        out_shape=[jax.ShapeDtypeStruct((2, NB_DEV * BLK, channels), dtype) for dtype in dtypes],
        in_specs=[pl.BlockSpec(memory_space=pltpu.SMEM)]
        + [pl.BlockSpec(memory_space=pl.ANY)] * (len(codes) + 4),
        out_specs=[pl.BlockSpec(memory_space=pltpu.VMEM)] * len(dtypes),
        scratch_shapes=[
            pltpu.VMEM((slots, BLK, BLK), jnp.int32),
            pltpu.VMEM((slots, BLK, channels), jnp.bfloat16),
            pltpu.VMEM((slots, BLK, channels), jnp.bfloat16),
            pltpu.VMEM((2, NB_DEV * BLK, channels), jnp.float32),
            pltpu.SemaphoreType.DMA((3, slots)),
        ],
        cost_estimate=pl.CostEstimate(flops=flops, bytes_accessed=moved, transcendentals=0),
        name="tile_products",
    )(meta, *codes, *blocks)


def project_kernel(chan_ref, p0, p1, p2, p3, enc_mix, dec_proj, node_embed, hidden, node_grad):
    chan = chan_ref[0]
    mixed = None
    for back, piece in enumerate((p0, p1, p2, p3)):
        rows = pl.ds(pl.multiple_of(((chan + CHAN - back) % CHAN) * 256, 256), 256)
        left = jnp.dot(piece[0], enc_mix[rows, :], preferred_element_type=jnp.float32)
        right = jnp.dot(piece[1], dec_proj[rows, :], preferred_element_type=jnp.float32)
        mixed, grad = (left, right) if mixed is None else (mixed + left, grad + right)
    hidden[...] = (node_embed[...].astype(jnp.float32) + mixed / (1.0 + jnp.exp(-mixed))).astype(hidden.dtype)
    node_grad[...] = grad.astype(node_grad.dtype)


def project(chan, pieces, enc_mix, dec_proj, node_embed):
    rows, channels = node_embed.shape
    vmem = pl.BlockSpec(memory_space=pltpu.VMEM)
    return pl.pallas_call(
        project_kernel,
        out_shape=[jax.ShapeDtypeStruct((rows, channels), jnp.bfloat16)] * 2,
        in_specs=[pl.BlockSpec(memory_space=pltpu.SMEM)] + [vmem] * 7,
        out_specs=[vmem] * 2,
        cost_estimate=pl.CostEstimate(
            flops=4 * rows * CHAN * channels * channels,
            bytes_accessed=4 * CHAN * rows * channels * 4,
            transcendentals=rows * channels,
        ),
        name="project",
    )(chan.reshape(1), *pieces, enc_mix, dec_proj, node_embed)


def near_step(band):
    return 1 - 2 * (band // 2 % 2)


def one_device(
    cells_next, node_embed, enc_mix, out_cotangent, decoded_saved, dec_proj, tile_source, tile_codes
):
    bands = lax.axis_size("band")
    band = lax.axis_index("band")
    chan = lax.axis_index("chan")
    core = band % 2
    tile_scale = (3.0 / (K * BLK)) ** 0.5 / 128.0
    channels = cells_next.shape[1]
    go = functools.partial(permute, bands=bands)
    codes = tile_codes.reshape(TILES, BLK, BLK)
    cells = cells_next.reshape(CB_DEV, BLK, channels)
    cotangent = out_cotangent.reshape(CB_DEV, BLK, channels)
    quarter = SIDE // CHAN

    cells_sib = go(cells, lambda b, c: (b ^ 1, c))
    cotangent_sib = go(cotangent, lambda b, c: (b ^ 1, c))

    near = near_step(band)
    far = far_step_traced(core)
    readers = band + jnp.array([0, 0, 0, 0, 2, -2, 0], jnp.int32) * near + jnp.array([0] * 6 + [2], jnp.int32) * far
    offsets = (
        jnp.array([1, -1, 0, 0, -1, 1, 0], jnp.int32) * near + jnp.array([0, 0, -1, 0, 0, 0, -1], jnp.int32) * far
    )
    tile, block = slot_table(tile_source, readers, offsets)

    wanted = lax.dynamic_slice_in_dim(tile[:2], (CHAN - 1 - chan) * quarter, quarter, 1)
    pick = jnp.maximum(jnp.concatenate([wanted.reshape(-1), tile[2, :CAP]]), 0)
    keep_codes, give_codes, far_codes = pick_tiles(pick, codes, (quarter, quarter, CAP))
    give_codes = go(give_codes, lambda b, c: (b - 2 * near_step(b), CHAN - 1 - c))
    keep_codes = go(keep_codes, lambda b, c: (b ^ 2, CHAN - 1 - c))
    far_codes = go(far_codes, lambda b, c: (b - 2 * far_step(b), c))

    def over_chan(x):
        return [x] + [go(x, lambda b, c, by=by: (b, (c + by) % CHAN)) for by in range(1, CHAN)]

    give_codes = over_chan(give_codes)
    keep_codes = over_chan(keep_codes)

    half = decoded_saved.shape[0] // 2
    dec_first = go(decoded_saved[:half], lambda b, c: (b, c ^ 2))
    cot_pair = go(out_cotangent, lambda b, c: (b, c ^ 1))
    dec_second = go(decoded_saved[half:], lambda b, c: (b, c ^ 2))

    def meta_of(row, index):
        node = jnp.where(tile[row] < 0, NB_DEV, tile[row] // K)
        own = (block[row] // CB_DEV == core).astype(jnp.int32)
        return jnp.stack([node, own, block[row] % CB_DEV, index])

    def pieces_meta(row):
        meta = meta_of(row, jnp.arange(SIDE, dtype=jnp.int32) % quarter)
        double = jnp.concatenate([meta, meta], axis=1)
        parts = [
            lax.dynamic_slice_in_dim(double, (chan + CHAN - i) * quarter, quarter, 1) for i in range(CHAN)
        ]
        return jnp.concatenate(parts, axis=1)

    blocks = (cells, cells_sib, cotangent, cotangent_sib)
    piece_group = [[(i, i * quarter, quarter) for i in range(CHAN)]]
    near_meta = jnp.concatenate(
        [meta_of(6, jnp.arange(SIDE, dtype=jnp.int32))[:, :CAP], meta_of(3, jnp.maximum(tile[3], 0))], axis=1
    )
    far_part, own_part = tile_products(
        near_meta, [far_codes, codes], blocks, [[(0, 0, CAP)], [(1, CAP, SIDE)]], [jnp.bfloat16, jnp.float32]
    )
    got_far = go(far_part, lambda b, c: (b + 2 * far_step(b), c))
    (give_part,) = tile_products(pieces_meta(5), give_codes, blocks, piece_group, [jnp.bfloat16])
    got_give = go(give_part, lambda b, c: (b - 4 * near_step(b), c))
    (keep_part,) = tile_products(pieces_meta(4), keep_codes, blocks, piece_group, [jnp.float32])
    crossing = (keep_part + got_give.astype(jnp.float32)).astype(jnp.bfloat16)
    got_keep = go(crossing, lambda b, c: (b ^ 2, c))
    summed = own_part + got_keep.astype(jnp.float32) + got_far.astype(jnp.float32)
    aggregates = (summed * tile_scale).astype(jnp.bfloat16)
    pieces = over_chan(aggregates)
    hidden_nodes, node_grad = project(chan, pieces, enc_mix, dec_proj, node_embed)

    w_dec_grad = projection_gradient(go, out_cotangent, decoded_saved, cot_pair, (dec_first, dec_second), bands)
    return (hidden_nodes, node_grad, w_dec_grad)


def far_step_traced(core):
    return 2 - 4 * core


def projection_gradient(go, cot, dec, cot_pair, dec_pair, bands):
    band, chan = lax.axis_index("band"), lax.axis_index("chan")
    along = bands // 16
    x, y, zh, core = band // (4 * along), band // along % 4, band // 2 % 2, band % 2
    channels = cot.shape[1]
    cells_total = cot.shape[0] * bands
    rows = channels // 16

    def outer(left, right):
        return lax.dot_general(left, right, (((0,), (0,)), ((), ())), preferred_element_type=jnp.float32)

    def outer_halves(left):
        half = left.shape[0] // 2
        return outer(left[:half], dec_pair[0]) + outer(left[half:], dec_pair[1])

    first = outer(cot, dec)
    whole = jnp.stack([first, outer(cot_pair, dec), outer_halves(cot), outer_halves(cot_pair)])
    halves = whole.reshape(4, 8, 2, rows, channels)
    own = lax.dynamic_index_in_dim(halves, core, 2, keepdims=False)
    other = lax.dynamic_index_in_dim(halves, 1 - core, 2, keepdims=False).astype(jnp.bfloat16)
    own = own + go(other, lambda b, c: (b ^ 1, c)).astype(jnp.float32)

    def take(i):
        return lax.dynamic_index_in_dim(own, i, 0, keepdims=False)

    share = take(x ^ chan)
    for by in range(1, 4):
        sent = take(((x + by) % 4) ^ chan).astype(jnp.bfloat16)
        share = share + go(sent, lambda b, c: ((b + by * 4 * along) % bands, c)).astype(jnp.float32)

    own = share.reshape(4, 2, rows, channels)
    share = take(y)
    for by in range(1, 4):
        sent = take((y + by) % 4)
        share = share + go(sent, lambda b, c: (b // 16 * 16 + (b % 16 + by * 4) % 16, c))

    def home(b, c):
        at_x, rest = b // 16, b % 16
        return (2 * (c // 2) + at_x % 2) * 16 + rest, c % 2 + 2 * (at_x // 2)

    def home_across(b, c):
        return home(b ^ 2, c)

    own = share
    return (go(take(zh), home) + go(take(1 - zh), home_across)) * cells_total ** (-0.5)


def solution(mesh):
    in_specs = (
        P("band", "chan"),
        P("band", "chan"),
        P(None, "chan"),
        P("band", "chan"),
        P("band", "chan"),
        P(None, "chan"),
        P(),
        P("band", None, None, None),
    )
    out_specs = (P("band", "chan"), P("band", "chan"), P("band", "chan"))
    return jax.shard_map(one_device, mesh=mesh, in_specs=in_specs, out_specs=out_specs, check_vma=False)
```

```python
import functools

import jax
import jax.numpy as jnp
from jax import lax
from jax.experimental import pallas as pl
from jax.experimental.pallas import tpu as pltpu
from jax.sharding import PartitionSpec as P


BLK = 128
K = 16
CB_DEV = 16
NB_DEV = 2
CAP = 8
CHAN = 4
TILES = NB_DEV * K
PAIR_BLOCKS = 2 * CB_DEV
SIDE = 2 * CAP


def permute(x, move, bands):
    pairs = []
    for band in range(bands):
        for chan in range(CHAN):
            to_band, to_chan = move(band, chan)
            if 0 <= to_band < bands:
                pairs.append((band * CHAN + chan, to_band * CHAN + to_chan))
    return lax.ppermute(x, ("band", "chan"), pairs)


def far_step(band):
    return 2 if band % 2 == 0 else -2


def slot_table(tile_source, readers, offsets):
    bands = tile_source.shape[0] // NB_DEV
    rows = tile_source.reshape(bands, TILES)[jnp.clip(readers, 0, bands - 1)]
    hit = (rows // PAIR_BLOCKS - (readers // 2)[:, None]) == offsets[:, None]
    earlier = jnp.tril(jnp.ones((TILES, TILES), jnp.int32), -1)
    rank = jnp.sum(hit.astype(jnp.int32)[:, None, :] * earlier[None], axis=2)
    code = (jnp.arange(TILES, dtype=jnp.int32) * PAIR_BLOCKS)[None] + rows % PAIR_BLOCKS + 1
    chosen = hit[:, None, :] & (rank[:, None, :] == jnp.arange(SIDE, dtype=jnp.int32)[None, :, None])
    packed = jnp.sum(jnp.where(chosen, code[:, None, :], 0), axis=2) - 1
    tile = jnp.where(packed < 0, -1, packed // PAIR_BLOCKS)
    block = jnp.where(packed < 0, 0, packed % PAIR_BLOCKS)
    return tile, block


def pick_kernel(place, rows, codes, give_out, keep_out, far_out, listed, sems):
    band, chan = place[0], place[1]
    chip = band // 2
    near = 1 - 2 * (chip % 2)
    far = 2 - 4 * (band % 2)
    first = (CHAN - 1 - chan) * (SIDE // CHAN)
    for i in range(3 * SIDE):
        listed[i] = 0

    def sort(tile, counts):
        offset = rows[tile // K, tile % K] // PAIR_BLOCKS - chip
        after = []
        for kind, (wanted, count) in enumerate(zip((-near, near, -far), counts)):
            hit = offset == wanted

            @pl.when(hit & (count < SIDE))
            def _(kind=kind, count=count):
                listed[kind * SIDE + count] = tile

            after.append(count + hit.astype(jnp.int32))
        return tuple(after)

    zero = jnp.int32(0)
    lax.fori_loop(0, TILES, sort, (zero, zero, zero))
    copies = []
    for kind, (out, start) in enumerate(((give_out, first), (keep_out, first), (far_out, 0))):
        for i in range(out.shape[0]):
            tile = listed[kind * SIDE + start + i]
            copies.append(pltpu.make_async_copy(codes.at[tile], out.at[i], sems.at[len(copies)]))
            copies[-1].start()
    for copy in copies:
        copy.wait()


def pick_tiles(place, rows, codes):
    counts = (SIDE // CHAN, SIDE // CHAN, CAP)
    smem = pl.BlockSpec(memory_space=pltpu.SMEM)
    return pl.pallas_call(
        pick_kernel,
        out_shape=[jax.ShapeDtypeStruct((count, BLK, BLK), codes.dtype) for count in counts],
        in_specs=[smem, smem, pl.BlockSpec(memory_space=pl.ANY)],
        out_specs=[pl.BlockSpec(memory_space=pltpu.VMEM)] * 3,
        scratch_shapes=[pltpu.SMEM((3 * SIDE,), jnp.int32), pltpu.SemaphoreType.DMA((sum(counts),))],
        cost_estimate=pl.CostEstimate(flops=10**8, bytes_accessed=2 * sum(counts) * BLK * BLK * 4, transcendentals=0),
        name="pick_tiles",
    )(place, rows, codes)


def products_kernel(groups, n_codes, *refs):
    meta = refs[0]
    codes = refs[1 : 1 + n_codes]
    cells_own, cells_sib, cot_own, cot_sib = refs[1 + n_codes : 5 + n_codes]
    outs = refs[5 + n_codes : 5 + n_codes + len(groups)]
    code_buf, cell_buf, cot_buf, total, sems = refs[5 + n_codes + len(groups) :]
    for parts in groups:
        for operand, first, count in parts:
            source = codes[operand]

            def begin(i, carry, first=first, source=source):
                slot = first + i
                pltpu.make_async_copy(source.at[meta[3, slot]], code_buf.at[slot], sems.at[0, slot]).start()
                local = meta[2, slot]

                @pl.when(meta[1, slot] == 1)
                def _():
                    pltpu.make_async_copy(cells_own.at[local], cell_buf.at[slot], sems.at[1, slot]).start()
                    pltpu.make_async_copy(cot_own.at[local], cot_buf.at[slot], sems.at[2, slot]).start()

                @pl.when(meta[1, slot] != 1)
                def _():
                    pltpu.make_async_copy(cells_sib.at[local], cell_buf.at[slot], sems.at[1, slot]).start()
                    pltpu.make_async_copy(cot_sib.at[local], cot_buf.at[slot], sems.at[2, slot]).start()

                return carry

            lax.fori_loop(0, count, begin, 0)

    for out, parts in zip(outs, groups):
        total[...] = jnp.zeros_like(total)
        first = parts[0][1]
        slots = sum(count for _, _, count in parts)

        def step(i, carry, first=first):
            enc_rows, dec_rows = [[], []], [[], []]
            base = first + i * 4
            for inner in range(4):
                slot = base + inner
                pltpu.make_async_copy(codes[0].at[0], code_buf.at[slot], sems.at[0, slot]).wait()
                pltpu.make_async_copy(cells_own.at[0], cell_buf.at[slot], sems.at[1, slot]).wait()
                pltpu.make_async_copy(cot_own.at[0], cot_buf.at[slot], sems.at[2, slot]).wait()
                words = code_buf[slot]
                enc = ((words & 255) - 128).astype(jnp.float32)
                dec = ((words >> 8) - 128).astype(jnp.float32)
                for node in range(NB_DEV):
                    keep = (meta[0, slot] == node).astype(jnp.float32)
                    enc_rows[node].append((enc * keep).astype(jnp.bfloat16))
                    dec_rows[node].append((dec * keep).astype(jnp.bfloat16))
            wide = [
                jnp.concatenate([jnp.concatenate(line, axis=1) for line in both], axis=0)
                for both in (enc_rows, dec_rows)
            ]
            cells = cell_buf[pl.ds(base, 4)].reshape(4 * BLK, -1)
            cots = cot_buf[pl.ds(base, 4)].reshape(4 * BLK, -1)
            total[0] += jnp.dot(wide[0], cells, preferred_element_type=jnp.float32)
            total[1] += jnp.dot(wide[1], cots, preferred_element_type=jnp.float32)
            return carry

        lax.fori_loop(0, slots // 4, step, 0)
        out[...] = total[...].astype(out.dtype)


def tile_products(meta, codes, blocks, groups, dtypes):
    slots = meta.shape[1]
    channels = blocks[0].shape[-1]
    flops = slots * 4 * BLK * BLK * channels
    moved = slots * (BLK * BLK * 4 + 2 * BLK * channels * 2)
    return pl.pallas_call(
        functools.partial(products_kernel, groups, len(codes)),
        out_shape=[jax.ShapeDtypeStruct((2, NB_DEV * BLK, channels), dtype) for dtype in dtypes],
        in_specs=[pl.BlockSpec(memory_space=pltpu.SMEM)]
        + [pl.BlockSpec(memory_space=pl.ANY)] * (len(codes) + 4),
        out_specs=[pl.BlockSpec(memory_space=pltpu.VMEM)] * len(dtypes),
        scratch_shapes=[
            pltpu.VMEM((slots, BLK, BLK), jnp.int32),
            pltpu.VMEM((slots, BLK, channels), jnp.bfloat16),
            pltpu.VMEM((slots, BLK, channels), jnp.bfloat16),
            pltpu.VMEM((2, NB_DEV * BLK, channels), jnp.float32),
            pltpu.SemaphoreType.DMA((3, slots)),
        ],
        cost_estimate=pl.CostEstimate(flops=flops, bytes_accessed=moved, transcendentals=0),
        name="tile_products",
    )(meta, *codes, *blocks)


def project_kernel(chan_ref, p0, p1, p2, p3, enc_mix, dec_proj, node_embed, hidden, node_grad):
    chan = chan_ref[0]
    mixed = None
    for back, piece in enumerate((p0, p1, p2, p3)):
        rows = pl.ds(pl.multiple_of(((chan + CHAN - back) % CHAN) * 256, 256), 256)
        left = jnp.dot(piece[0], enc_mix[rows, :], preferred_element_type=jnp.float32)
        right = jnp.dot(piece[1], dec_proj[rows, :], preferred_element_type=jnp.float32)
        mixed, grad = (left, right) if mixed is None else (mixed + left, grad + right)
    hidden[...] = (node_embed[...].astype(jnp.float32) + mixed / (1.0 + jnp.exp(-mixed))).astype(hidden.dtype)
    node_grad[...] = grad.astype(node_grad.dtype)


def project(chan, pieces, enc_mix, dec_proj, node_embed):
    rows, channels = node_embed.shape
    vmem = pl.BlockSpec(memory_space=pltpu.VMEM)
    return pl.pallas_call(
        project_kernel,
        out_shape=[jax.ShapeDtypeStruct((rows, channels), jnp.bfloat16)] * 2,
        in_specs=[pl.BlockSpec(memory_space=pltpu.SMEM)] + [vmem] * 7,
        out_specs=[vmem] * 2,
        cost_estimate=pl.CostEstimate(
            flops=4 * rows * CHAN * channels * channels,
            bytes_accessed=4 * CHAN * rows * channels * 4,
            transcendentals=rows * channels,
        ),
        name="project",
    )(chan.reshape(1), *pieces, enc_mix, dec_proj, node_embed)


def near_step(band):
    return 1 - 2 * (band // 2 % 2)


def one_device(
    cells_next, node_embed, enc_mix, out_cotangent, decoded_saved, dec_proj, tile_source, tile_codes
):
    bands = lax.axis_size("band")
    band = lax.axis_index("band")
    chan = lax.axis_index("chan")
    core = band % 2
    tile_scale = (3.0 / (K * BLK)) ** 0.5 / 128.0
    channels = cells_next.shape[1]
    go = functools.partial(permute, bands=bands)
    codes = tile_codes.reshape(TILES, BLK, BLK)
    cells = cells_next.reshape(CB_DEV, BLK, channels)
    cotangent = out_cotangent.reshape(CB_DEV, BLK, channels)
    quarter = SIDE // CHAN

    cells_sib = go(cells, lambda b, c: (b ^ 1, c))
    cotangent_sib = go(cotangent, lambda b, c: (b ^ 1, c))

    rows = lax.dynamic_slice_in_dim(tile_source, band * NB_DEV, NB_DEV, 0)
    place = jnp.stack([band, chan]).astype(jnp.int32)
    give_codes, keep_codes, far_codes = pick_tiles(place, rows, codes)
    give_codes = go(give_codes, lambda b, c: (b - 2 * near_step(b), CHAN - 1 - c))
    keep_codes = go(keep_codes, lambda b, c: (b ^ 2, CHAN - 1 - c))
    far_codes = go(far_codes, lambda b, c: (b - 2 * far_step(b), c))

    def over_chan(x):
        return [x] + [go(x, lambda b, c, by=by: (b, (c + by) % CHAN)) for by in range(1, CHAN)]

    give_codes = over_chan(give_codes)
    keep_codes = over_chan(keep_codes)

    dec_pair = go(decoded_saved, lambda b, c: (b, c ^ 2))
    cot_pair = go(out_cotangent, lambda b, c: (b, c ^ 1))

    near = near_step(band)
    far = far_step_traced(core)
    readers = band + jnp.array([2, -2, 0, 0], jnp.int32) * near + jnp.array([0, 0, 2, 0], jnp.int32) * far
    offsets = jnp.array([-1, 1, 0, 0], jnp.int32) * near + jnp.array([0, 0, -1, 0], jnp.int32) * far
    tile, block = slot_table(tile_source, readers, offsets)

    def meta_of(row, index):
        node = jnp.where(tile[row] < 0, NB_DEV, tile[row] // K)
        own = (block[row] // CB_DEV == core).astype(jnp.int32)
        return jnp.stack([node, own, block[row] % CB_DEV, index])

    def pieces_meta(row):
        meta = meta_of(row, jnp.arange(SIDE, dtype=jnp.int32) % quarter)
        double = jnp.concatenate([meta, meta], axis=1)
        parts = [
            lax.dynamic_slice_in_dim(double, (chan + CHAN - i) * quarter, quarter, 1) for i in range(CHAN)
        ]
        return jnp.concatenate(parts, axis=1)

    blocks = (cells, cells_sib, cotangent, cotangent_sib)
    piece_group = [[(i, i * quarter, quarter) for i in range(CHAN)]]
    near_meta = jnp.concatenate(
        [meta_of(2, jnp.arange(SIDE, dtype=jnp.int32))[:, :CAP], meta_of(3, jnp.maximum(tile[3], 0))], axis=1
    )
    far_part, own_part = tile_products(
        near_meta, [far_codes, codes], blocks, [[(0, 0, CAP)], [(1, CAP, SIDE)]], [jnp.bfloat16, jnp.float32]
    )
    got_far = go(far_part, lambda b, c: (b + 2 * far_step(b), c))
    (give_part,) = tile_products(pieces_meta(1), give_codes, blocks, piece_group, [jnp.bfloat16])
    got_give = go(give_part, lambda b, c: (b - 4 * near_step(b), c))
    (keep_part,) = tile_products(pieces_meta(0), keep_codes, blocks, piece_group, [jnp.float32])
    crossing = (keep_part + got_give.astype(jnp.float32)).astype(jnp.bfloat16)
    got_keep = go(crossing, lambda b, c: (b ^ 2, c))
    summed = own_part + got_keep.astype(jnp.float32) + got_far.astype(jnp.float32)
    aggregates = (summed * tile_scale).astype(jnp.bfloat16)
    pieces = over_chan(aggregates)
    hidden_nodes, node_grad = project(chan, pieces, enc_mix, dec_proj, node_embed)

    w_dec_grad = projection_gradient(go, out_cotangent, decoded_saved, cot_pair, dec_pair, bands)
    return (hidden_nodes, node_grad, w_dec_grad)


def far_step_traced(core):
    return 2 - 4 * core


def projection_gradient(go, cot, dec, cot_pair, dec_pair, bands):
    band, chan = lax.axis_index("band"), lax.axis_index("chan")
    along = bands // 16
    x, y, zh, core = band // (4 * along), band // along % 4, band // 2 % 2, band % 2
    channels = cot.shape[1]
    cells_total = cot.shape[0] * bands
    rows = channels // 16

    def outer(left, right):
        return lax.dot_general(left, right, (((0,), (0,)), ((), ())), preferred_element_type=jnp.float32)

    first = outer(cot, dec)
    third = outer(cot, dec_pair)
    second, fourth = outer(cot_pair, dec), outer(cot_pair, dec_pair)
    whole = jnp.stack([first, second, third, fourth])
    halves = whole.reshape(4, 8, 2, rows, channels)
    own = lax.dynamic_index_in_dim(halves, core, 2, keepdims=False)
    other = lax.dynamic_index_in_dim(halves, 1 - core, 2, keepdims=False).astype(jnp.bfloat16)
    own = own + go(other, lambda b, c: (b ^ 1, c)).astype(jnp.float32)

    def take(i):
        return lax.dynamic_index_in_dim(own, i, 0, keepdims=False)

    share = take(x ^ chan)
    for by in range(1, 4):
        sent = take(((x + by) % 4) ^ chan).astype(jnp.bfloat16)
        share = share + go(sent, lambda b, c: ((b + by * 4 * along) % bands, c)).astype(jnp.float32)

    own = share.reshape(4, 2, rows, channels)
    share = take(y)
    for by in range(1, 4):
        sent = take((y + by) % 4)
        share = share + go(sent, lambda b, c: (b // 16 * 16 + (b % 16 + by * 4) % 16, c))

    def home(b, c):
        at_x, rest = b // 16, b % 16
        return (2 * (c // 2) + at_x % 2) * 16 + rest, c % 2 + 2 * (at_x // 2)

    def home_across(b, c):
        return home(b ^ 2, c)

    own = share
    return (go(take(zh), home) + go(take(1 - zh), home_across)) * cells_total ** (-0.5)


def solution(mesh):
    in_specs = (
        P("band", "chan"),
        P("band", "chan"),
        P(None, "chan"),
        P("band", "chan"),
        P("band", "chan"),
        P(None, "chan"),
        P(),
        P("band", None, None, None),
    )
    out_specs = (P("band", "chan"), P("band", "chan"), P("band", "chan"))
    return jax.shard_map(one_device, mesh=mesh, in_specs=in_specs, out_specs=out_specs, check_vma=False)
```

```python
import functools

import jax
import jax.numpy as jnp
from jax import lax
from jax.experimental import pallas as pl
from jax.experimental.pallas import tpu as pltpu
from jax.sharding import PartitionSpec as P


BLK = 128
K = 16
CB_DEV = 16
NB_DEV = 2
CAP = 8
CHAN = 4
TILES = NB_DEV * K
PAIR_BLOCKS = 2 * CB_DEV
SIDE = 2 * CAP


def permute(x, move, bands):
    pairs = []
    for band in range(bands):
        for chan in range(CHAN):
            to_band, to_chan = move(band, chan)
            if 0 <= to_band < bands and 0 <= to_chan < CHAN:
                pairs.append((band * CHAN + chan, to_band * CHAN + to_chan))
    return lax.ppermute(x, ("band", "chan"), pairs)


def far_step(band):
    return 2 if band % 2 == 0 else -2


def slot_table(tile_source, readers, offsets):
    bands = tile_source.shape[0] // NB_DEV
    rows = tile_source.reshape(bands, TILES)[jnp.clip(readers, 0, bands - 1)]
    hit = (rows // PAIR_BLOCKS - (readers // 2)[:, None]) == offsets[:, None]
    earlier = jnp.tril(jnp.ones((TILES, TILES), jnp.int32), -1)
    rank = jnp.sum(hit.astype(jnp.int32)[:, None, :] * earlier[None], axis=2)
    code = (jnp.arange(TILES, dtype=jnp.int32) * PAIR_BLOCKS)[None] + rows % PAIR_BLOCKS + 1
    chosen = hit[:, None, :] & (rank[:, None, :] == jnp.arange(SIDE, dtype=jnp.int32)[None, :, None])
    packed = jnp.sum(jnp.where(chosen, code[:, None, :], 0), axis=2) - 1
    tile = jnp.where(packed < 0, -1, packed // PAIR_BLOCKS)
    block = jnp.where(packed < 0, 0, packed % PAIR_BLOCKS)
    return tile, block


def pick_kernel(place, rows, codes, give_out, keep_out, give_extra, keep_extra, far_out, listed, sems):
    band, chan = place[0], place[1]
    chip = band // 2
    near = 1 - 2 * (chip % 2)
    far = 2 - 4 * (band % 2)
    first = (CHAN - 1 - chan) * (SIDE // CHAN)
    extra = chan * (SIDE // CHAN)
    for i in range(3 * SIDE):
        listed[i] = 0

    def sort(tile, counts):
        offset = rows[tile // K, tile % K] // PAIR_BLOCKS - chip
        after = []
        for kind, (wanted, count) in enumerate(zip((-near, near, -far), counts)):
            hit = offset == wanted

            @pl.when(hit & (count < SIDE))
            def _(kind=kind, count=count):
                listed[kind * SIDE + count] = tile

            after.append(count + hit.astype(jnp.int32))
        return tuple(after)

    zero = jnp.int32(0)
    lax.fori_loop(0, TILES, sort, (zero, zero, zero))
    copies = []
    picks = ((0, give_out, first), (1, keep_out, first), (0, give_extra, extra), (1, keep_extra, extra), (2, far_out, 0))
    for kind, out, start in picks:
        for i in range(out.shape[0]):
            tile = listed[kind * SIDE + start + i]
            copies.append(pltpu.make_async_copy(codes.at[tile], out.at[i], sems.at[len(copies)]))
            copies[-1].start()
    for copy in copies:
        copy.wait()


def pick_tiles(place, rows, codes):
    counts = (SIDE // CHAN,) * 4 + (CAP,)
    smem = pl.BlockSpec(memory_space=pltpu.SMEM)
    return pl.pallas_call(
        pick_kernel,
        out_shape=[jax.ShapeDtypeStruct((count, BLK, BLK), codes.dtype) for count in counts],
        in_specs=[smem, smem, pl.BlockSpec(memory_space=pl.ANY)],
        out_specs=[pl.BlockSpec(memory_space=pltpu.VMEM)] * len(counts),
        scratch_shapes=[pltpu.SMEM((3 * SIDE,), jnp.int32), pltpu.SemaphoreType.DMA((sum(counts),))],
        cost_estimate=pl.CostEstimate(flops=10**8, bytes_accessed=2 * sum(counts) * BLK * BLK * 4, transcendentals=0),
        name="pick_tiles",
    )(place, rows, codes)


def products_kernel(groups, n_codes, *refs):
    meta = refs[0]
    codes = refs[1 : 1 + n_codes]
    cells_own, cells_sib, cot_own, cot_sib = refs[1 + n_codes : 5 + n_codes]
    outs = refs[5 + n_codes : 5 + n_codes + len(groups)]
    code_buf, cell_buf, cot_buf, total, sems = refs[5 + n_codes + len(groups) :]
    for parts in groups:
        for operands, first, count in parts:

            def begin(i, carry, first=first, operands=operands):
                slot = first + i
                for operand in operands:

                    @pl.when((meta[4, slot] == operand) | (len(operands) == 1))
                    def _(operand=operand):
                        pltpu.make_async_copy(
                            codes[operand].at[meta[3, slot]], code_buf.at[slot], sems.at[0, slot]
                        ).start()

                local = meta[2, slot]

                @pl.when(meta[1, slot] == 1)
                def _():
                    pltpu.make_async_copy(cells_own.at[local], cell_buf.at[slot], sems.at[1, slot]).start()
                    pltpu.make_async_copy(cot_own.at[local], cot_buf.at[slot], sems.at[2, slot]).start()

                @pl.when(meta[1, slot] != 1)
                def _():
                    pltpu.make_async_copy(cells_sib.at[local], cell_buf.at[slot], sems.at[1, slot]).start()
                    pltpu.make_async_copy(cot_sib.at[local], cot_buf.at[slot], sems.at[2, slot]).start()

                return carry

            lax.fori_loop(0, count, begin, 0)

    for out, parts in zip(outs, groups):
        total[...] = jnp.zeros_like(total)
        first = parts[0][1]
        slots = sum(count for _, _, count in parts)

        def step(i, carry, first=first):
            enc_rows, dec_rows = [[], []], [[], []]
            base = first + i * 4
            for inner in range(4):
                slot = base + inner
                pltpu.make_async_copy(codes[0].at[0], code_buf.at[slot], sems.at[0, slot]).wait()
                pltpu.make_async_copy(cells_own.at[0], cell_buf.at[slot], sems.at[1, slot]).wait()
                pltpu.make_async_copy(cot_own.at[0], cot_buf.at[slot], sems.at[2, slot]).wait()
                words = code_buf[slot]
                enc = ((words & 255) - 128).astype(jnp.float32)
                dec = ((words >> 8) - 128).astype(jnp.float32)
                for node in range(NB_DEV):
                    keep = (meta[0, slot] == node).astype(jnp.float32)
                    enc_rows[node].append((enc * keep).astype(jnp.bfloat16))
                    dec_rows[node].append((dec * keep).astype(jnp.bfloat16))
            wide = [
                jnp.concatenate([jnp.concatenate(line, axis=1) for line in both], axis=0)
                for both in (enc_rows, dec_rows)
            ]
            cells = cell_buf[pl.ds(base, 4)].reshape(4 * BLK, -1)
            cots = cot_buf[pl.ds(base, 4)].reshape(4 * BLK, -1)
            total[0] += jnp.dot(wide[0], cells, preferred_element_type=jnp.float32)
            total[1] += jnp.dot(wide[1], cots, preferred_element_type=jnp.float32)
            return carry

        lax.fori_loop(0, slots // 4, step, 0)
        out[...] = total[...].astype(out.dtype)


def tile_products(meta, codes, blocks, groups, dtypes):
    slots = meta.shape[1]
    channels = blocks[0].shape[-1]
    flops = slots * 4 * BLK * BLK * channels
    moved = slots * (BLK * BLK * 4 + 2 * BLK * channels * 2)
    return pl.pallas_call(
        functools.partial(products_kernel, groups, len(codes)),
        out_shape=[jax.ShapeDtypeStruct((2, NB_DEV * BLK, channels), dtype) for dtype in dtypes],
        in_specs=[pl.BlockSpec(memory_space=pltpu.SMEM)]
        + [pl.BlockSpec(memory_space=pl.ANY)] * (len(codes) + 4),
        out_specs=[pl.BlockSpec(memory_space=pltpu.VMEM)] * len(dtypes),
        scratch_shapes=[
            pltpu.VMEM((slots, BLK, BLK), jnp.int32),
            pltpu.VMEM((slots, BLK, channels), jnp.bfloat16),
            pltpu.VMEM((slots, BLK, channels), jnp.bfloat16),
            pltpu.VMEM((2, NB_DEV * BLK, channels), jnp.float32),
            pltpu.SemaphoreType.DMA((3, slots)),
        ],
        cost_estimate=pl.CostEstimate(flops=flops, bytes_accessed=moved, transcendentals=0),
        name="tile_products",
    )(meta, *codes, *blocks)


def project_kernel(chan_ref, p0, p1, p2, p3, enc_mix, dec_proj, node_embed, hidden, node_grad):
    chan = chan_ref[0]
    mixed = None
    for back, piece in enumerate((p0, p1, p2, p3)):
        rows = pl.ds(pl.multiple_of(((chan + CHAN - back) % CHAN) * 256, 256), 256)
        left = jnp.dot(piece[0], enc_mix[rows, :], preferred_element_type=jnp.float32)
        right = jnp.dot(piece[1], dec_proj[rows, :], preferred_element_type=jnp.float32)
        mixed, grad = (left, right) if mixed is None else (mixed + left, grad + right)
    hidden[...] = (node_embed[...].astype(jnp.float32) + mixed / (1.0 + jnp.exp(-mixed))).astype(hidden.dtype)
    node_grad[...] = grad.astype(node_grad.dtype)


def project(chan, pieces, enc_mix, dec_proj, node_embed):
    rows, channels = node_embed.shape
    vmem = pl.BlockSpec(memory_space=pltpu.VMEM)
    return pl.pallas_call(
        project_kernel,
        out_shape=[jax.ShapeDtypeStruct((rows, channels), jnp.bfloat16)] * 2,
        in_specs=[pl.BlockSpec(memory_space=pltpu.SMEM)] + [vmem] * 7,
        out_specs=[vmem] * 2,
        cost_estimate=pl.CostEstimate(
            flops=4 * rows * CHAN * channels * channels,
            bytes_accessed=4 * CHAN * rows * channels * 4,
            transcendentals=rows * channels,
        ),
        name="project",
    )(chan.reshape(1), *pieces, enc_mix, dec_proj, node_embed)


def near_step(band):
    return 1 - 2 * (band // 2 % 2)


def one_device(
    cells_next, node_embed, enc_mix, out_cotangent, decoded_saved, dec_proj, tile_source, tile_codes
):
    bands = lax.axis_size("band")
    band = lax.axis_index("band")
    chan = lax.axis_index("chan")
    core = band % 2
    tile_scale = (3.0 / (K * BLK)) ** 0.5 / 128.0
    channels = cells_next.shape[1]
    go = functools.partial(permute, bands=bands)
    codes = tile_codes.reshape(TILES, BLK, BLK)
    cells = cells_next.reshape(CB_DEV, BLK, channels)
    cotangent = out_cotangent.reshape(CB_DEV, BLK, channels)
    quarter = SIDE // CHAN

    cells_sib = go(cells, lambda b, c: (b ^ 1, c))
    cotangent_sib = go(cotangent, lambda b, c: (b ^ 1, c))

    rows = lax.dynamic_slice_in_dim(tile_source, band * NB_DEV, NB_DEV, 0)
    place = jnp.stack([band, chan]).astype(jnp.int32)
    give_codes, keep_codes, give_extra, keep_extra, far_codes = pick_tiles(place, rows, codes)
    ends = (0, CHAN - 1)

    def mirrored(c):
        return CHAN - 1 - c

    def if_end(c):
        return mirrored(c) if c in ends else -1

    give_codes = go(give_codes, lambda b, c: (b - 2 * near_step(b), mirrored(c)))
    keep_codes = go(keep_codes, lambda b, c: (b ^ 2, mirrored(c)))
    give_extra = go(give_extra, lambda b, c: (b - 2 * near_step(b), if_end(c)))
    keep_extra = go(keep_extra, lambda b, c: (b ^ 2, if_end(c)))
    far_codes = go(far_codes, lambda b, c: (b - 2 * far_step(b), c))

    def by_relay(x, extra):
        up = go(x, lambda b, c: (b, c + 1))
        down = go(x, lambda b, c: (b, c - 1))
        up_up = go(up, lambda b, c: (b, c + 1 if c > 0 else -1))
        down_down = go(down, lambda b, c: (b, c - 1 if c < CHAN - 1 else -1))
        return [x, up, down, up_up, down_down, extra]

    give_codes = by_relay(give_codes, give_extra)
    keep_codes = by_relay(keep_codes, keep_extra)

    def over_chan(x):
        return [x] + [go(x, lambda b, c, by=by: (b, (c + by) % CHAN)) for by in range(1, CHAN)]

    dec_pair = go(decoded_saved, lambda b, c: (b, c ^ 2))
    cot_pair = go(out_cotangent, lambda b, c: (b, c ^ 1))

    near = near_step(band)
    far = far_step_traced(core)
    readers = band + jnp.array([2, -2, 0, 0], jnp.int32) * near + jnp.array([0, 0, 2, 0], jnp.int32) * far
    offsets = jnp.array([-1, 1, 0, 0], jnp.int32) * near + jnp.array([0, 0, -1, 0], jnp.int32) * far
    tile, block = slot_table(tile_source, readers, offsets)

    slots = jnp.arange(SIDE, dtype=jnp.int32)

    def meta_of(row, index):
        node = jnp.where(tile[row] < 0, NB_DEV, tile[row] // K)
        own = (block[row] // CB_DEV == core).astype(jnp.int32)
        away = slots // quarter - chan
        operand = jnp.where(away < 0, -2 * away - 1, 2 * away)
        operand = jnp.where(jnp.abs(away) == CHAN - 1, 5, operand)
        return jnp.stack([node, own, block[row] % CB_DEV, index, operand])

    def pieces_meta(row):
        return meta_of(row, slots % quarter)

    blocks = (cells, cells_sib, cotangent, cotangent_sib)
    piece_group = [[(tuple(range(6)), 0, SIDE)]]
    near_meta = jnp.concatenate([meta_of(2, slots)[:, :CAP], meta_of(3, jnp.maximum(tile[3], 0))], axis=1)
    far_part, own_part = tile_products(
        near_meta, [far_codes, codes], blocks, [[((0,), 0, CAP)], [((1,), CAP, SIDE)]], [jnp.bfloat16, jnp.float32]
    )
    got_far = go(far_part, lambda b, c: (b + 2 * far_step(b), c))
    (give_part,) = tile_products(pieces_meta(1), give_codes, blocks, piece_group, [jnp.bfloat16])
    got_give = go(give_part, lambda b, c: (b - 4 * near_step(b), c))
    (keep_part,) = tile_products(pieces_meta(0), keep_codes, blocks, piece_group, [jnp.float32])
    crossing = (keep_part + got_give.astype(jnp.float32)).astype(jnp.bfloat16)
    got_keep = go(crossing, lambda b, c: (b ^ 2, c))
    summed = own_part + got_keep.astype(jnp.float32) + got_far.astype(jnp.float32)
    aggregates = (summed * tile_scale).astype(jnp.bfloat16)
    pieces = over_chan(aggregates)
    hidden_nodes, node_grad = project(chan, pieces, enc_mix, dec_proj, node_embed)

    w_dec_grad = projection_gradient(go, out_cotangent, decoded_saved, cot_pair, dec_pair, bands)
    return (hidden_nodes, node_grad, w_dec_grad)


def far_step_traced(core):
    return 2 - 4 * core


def projection_gradient(go, cot, dec, cot_pair, dec_pair, bands):
    band, chan = lax.axis_index("band"), lax.axis_index("chan")
    along = bands // 16
    x, y, zh, core = band // (4 * along), band // along % 4, band // 2 % 2, band % 2
    channels = cot.shape[1]
    cells_total = cot.shape[0] * bands
    rows = channels // 16

    def outer(left, right):
        return lax.dot_general(left, right, (((0,), (0,)), ((), ())), preferred_element_type=jnp.float32)

    first = outer(cot, dec)
    third = outer(cot, dec_pair)
    second, fourth = outer(cot_pair, dec), outer(cot_pair, dec_pair)
    whole = jnp.stack([first, second, third, fourth])
    halves = whole.reshape(4, 8, 2, rows, channels)
    own = lax.dynamic_index_in_dim(halves, core, 2, keepdims=False)
    other = lax.dynamic_index_in_dim(halves, 1 - core, 2, keepdims=False).astype(jnp.bfloat16)
    own = own + go(other, lambda b, c: (b ^ 1, c)).astype(jnp.float32)

    def take(i):
        return lax.dynamic_index_in_dim(own, i, 0, keepdims=False)

    share = take(x ^ chan)
    for by in range(1, 4):
        sent = take(((x + by) % 4) ^ chan).astype(jnp.bfloat16)
        share = share + go(sent, lambda b, c: ((b + by * 4 * along) % bands, c)).astype(jnp.float32)

    own = share.reshape(4, 2, rows, channels)
    share = take(y)
    for by in range(1, 4):
        sent = take((y + by) % 4)
        share = share + go(sent, lambda b, c: (b // 16 * 16 + (b % 16 + by * 4) % 16, c))

    def home(b, c):
        at_x, rest = b // 16, b % 16
        return (2 * (c // 2) + at_x % 2) * 16 + rest, c % 2 + 2 * (at_x // 2)

    def home_across(b, c):
        return home(b ^ 2, c)

    own = share
    return (go(take(zh), home) + go(take(1 - zh), home_across)) * cells_total ** (-0.5)


def solution(mesh):
    in_specs = (
        P("band", "chan"),
        P("band", "chan"),
        P(None, "chan"),
        P("band", "chan"),
        P("band", "chan"),
        P(None, "chan"),
        P(),
        P("band", None, None, None),
    )
    out_specs = (P("band", "chan"), P("band", "chan"), P("band", "chan"))
    return jax.shard_map(one_device, mesh=mesh, in_specs=in_specs, out_specs=out_specs, check_vma=False)
```

```python
import functools

import jax
import jax.numpy as jnp
from jax import lax
from jax.experimental import pallas as pl
from jax.experimental.pallas import tpu as pltpu
from jax.sharding import PartitionSpec as P


BLK = 128
K = 16
CB_DEV = 16
NB_DEV = 2
CAP = 8
CHAN = 4
TILES = NB_DEV * K
PAIR_BLOCKS = 2 * CB_DEV
SIDE = 2 * CAP


def permute(x, move, bands):
    pairs = []
    for band in range(bands):
        for chan in range(CHAN):
            to_band, to_chan = move(band, chan)
            if 0 <= to_band < bands and 0 <= to_chan < CHAN:
                pairs.append((band * CHAN + chan, to_band * CHAN + to_chan))
    return lax.ppermute(x, ("band", "chan"), pairs)


def far_step(band):
    return 2 if band % 2 == 0 else -2


def slot_table(tile_source, readers, offsets):
    bands = tile_source.shape[0] // NB_DEV
    rows = tile_source.reshape(bands, TILES)[jnp.clip(readers, 0, bands - 1)]
    hit = (rows // PAIR_BLOCKS - (readers // 2)[:, None]) == offsets[:, None]
    earlier = jnp.tril(jnp.ones((TILES, TILES), jnp.int32), -1)
    rank = jnp.sum(hit.astype(jnp.int32)[:, None, :] * earlier[None], axis=2)
    code = (jnp.arange(TILES, dtype=jnp.int32) * PAIR_BLOCKS)[None] + rows % PAIR_BLOCKS + 1
    chosen = hit[:, None, :] & (rank[:, None, :] == jnp.arange(SIDE, dtype=jnp.int32)[None, :, None])
    packed = jnp.sum(jnp.where(chosen, code[:, None, :], 0), axis=2) - 1
    tile = jnp.where(packed < 0, -1, packed // PAIR_BLOCKS)
    block = jnp.where(packed < 0, 0, packed % PAIR_BLOCKS)
    return tile, block


def pick_kernel(picks, place, rows, codes, *refs):
    outs, (listed, sems) = refs[:-2], refs[-2:]
    band, chan = place[0], place[1]
    chip = band // 2
    near = 1 - 2 * (chip % 2)
    far = 2 - 4 * (band % 2)
    starts = {"mirrored": (CHAN - 1 - chan) * (SIDE // CHAN), "own": chan * (SIDE // CHAN), "all": 0}
    for i in range(3 * SIDE):
        listed[i] = 0

    def sort(tile, counts):
        offset = rows[tile % K, band * NB_DEV + tile // K] // PAIR_BLOCKS - chip
        after = []
        for kind, (wanted, count) in enumerate(zip((-near, near, -far), counts)):
            hit = offset == wanted

            @pl.when(hit & (count < SIDE))
            def _(kind=kind, count=count):
                listed[kind * SIDE + count] = tile

            after.append(count + hit.astype(jnp.int32))
        return tuple(after)

    zero = jnp.int32(0)
    lax.fori_loop(0, TILES, sort, (zero, zero, zero))
    copies = []
    for out, (kind, which) in zip(outs, picks):
        for i in range(out.shape[0]):
            tile = listed[kind * SIDE + starts[which] + i]
            copies.append(pltpu.make_async_copy(codes.at[tile], out.at[i], sems.at[len(copies)]))
            copies[-1].start()
    for copy in copies:
        copy.wait()


def pick_tiles(place, rows, codes, picks):
    counts = [CAP if which == "all" else SIDE // CHAN for _, which in picks]
    smem = pl.BlockSpec(memory_space=pltpu.SMEM)
    return pl.pallas_call(
        functools.partial(pick_kernel, picks),
        out_shape=[jax.ShapeDtypeStruct((count, BLK, BLK), codes.dtype) for count in counts],
        in_specs=[smem, smem, pl.BlockSpec(memory_space=pl.ANY)],
        out_specs=[pl.BlockSpec(memory_space=pltpu.VMEM)] * len(counts),
        scratch_shapes=[pltpu.SMEM((3 * SIDE,), jnp.int32), pltpu.SemaphoreType.DMA((sum(counts),))],
        cost_estimate=pl.CostEstimate(flops=10**8, bytes_accessed=2 * sum(counts) * BLK * BLK * 4, transcendentals=0),
        name="pick_tiles",
    )(place, rows, codes)


def products_kernel(groups, n_codes, *refs):
    meta = refs[0]
    codes = refs[1 : 1 + n_codes]
    cells_own, cells_sib, cot_own, cot_sib = refs[1 + n_codes : 5 + n_codes]
    outs = refs[5 + n_codes : 5 + n_codes + len(groups)]
    code_buf, cell_buf, cot_buf, total, sems = refs[5 + n_codes + len(groups) :]
    for parts in groups:
        for operands, first, count in parts:

            def begin(i, carry, first=first, operands=operands):
                slot = first + i
                for operand in operands:

                    @pl.when((meta[4, slot] == operand) | (len(operands) == 1))
                    def _(operand=operand):
                        pltpu.make_async_copy(
                            codes[operand].at[meta[3, slot]], code_buf.at[slot], sems.at[0, slot]
                        ).start()

                local = meta[2, slot]

                @pl.when(meta[1, slot] == 1)
                def _():
                    pltpu.make_async_copy(cells_own.at[local], cell_buf.at[slot], sems.at[1, slot]).start()
                    pltpu.make_async_copy(cot_own.at[local], cot_buf.at[slot], sems.at[2, slot]).start()

                @pl.when(meta[1, slot] != 1)
                def _():
                    pltpu.make_async_copy(cells_sib.at[local], cell_buf.at[slot], sems.at[1, slot]).start()
                    pltpu.make_async_copy(cot_sib.at[local], cot_buf.at[slot], sems.at[2, slot]).start()

                return carry

            lax.fori_loop(0, count, begin, 0)

    for out, parts in zip(outs, groups):
        total[...] = jnp.zeros_like(total)
        first = parts[0][1]
        slots = sum(count for _, _, count in parts)

        def step(i, carry, first=first):
            enc_rows, dec_rows = [[], []], [[], []]
            base = first + i * 4
            for inner in range(4):
                slot = base + inner
                pltpu.make_async_copy(codes[0].at[0], code_buf.at[slot], sems.at[0, slot]).wait()
                pltpu.make_async_copy(cells_own.at[0], cell_buf.at[slot], sems.at[1, slot]).wait()
                pltpu.make_async_copy(cot_own.at[0], cot_buf.at[slot], sems.at[2, slot]).wait()
                words = code_buf[slot]
                enc = ((words & 255) - 128).astype(jnp.float32)
                dec = ((words >> 8) - 128).astype(jnp.float32)
                for node in range(NB_DEV):
                    keep = (meta[0, slot] == node).astype(jnp.float32)
                    enc_rows[node].append((enc * keep).astype(jnp.bfloat16))
                    dec_rows[node].append((dec * keep).astype(jnp.bfloat16))
            wide = [
                jnp.concatenate([jnp.concatenate(line, axis=1) for line in both], axis=0)
                for both in (enc_rows, dec_rows)
            ]
            cells = cell_buf[pl.ds(base, 4)].reshape(4 * BLK, -1)
            cots = cot_buf[pl.ds(base, 4)].reshape(4 * BLK, -1)
            total[0] += jnp.dot(wide[0], cells, preferred_element_type=jnp.float32)
            total[1] += jnp.dot(wide[1], cots, preferred_element_type=jnp.float32)
            return carry

        lax.fori_loop(0, slots // 4, step, 0)
        out[...] = total[...].astype(out.dtype)


def tile_products(meta, codes, blocks, groups, dtypes):
    slots = meta.shape[1]
    channels = blocks[0].shape[-1]
    flops = slots * 4 * BLK * BLK * channels
    moved = slots * (BLK * BLK * 4 + 2 * BLK * channels * 2)
    return pl.pallas_call(
        functools.partial(products_kernel, groups, len(codes)),
        out_shape=[jax.ShapeDtypeStruct((2, NB_DEV * BLK, channels), dtype) for dtype in dtypes],
        in_specs=[pl.BlockSpec(memory_space=pltpu.SMEM)]
        + [pl.BlockSpec(memory_space=pl.ANY)] * (len(codes) + 4),
        out_specs=[pl.BlockSpec(memory_space=pltpu.VMEM)] * len(dtypes),
        scratch_shapes=[
            pltpu.VMEM((slots, BLK, BLK), jnp.int32),
            pltpu.VMEM((slots, BLK, channels), jnp.bfloat16),
            pltpu.VMEM((slots, BLK, channels), jnp.bfloat16),
            pltpu.VMEM((2, NB_DEV * BLK, channels), jnp.float32),
            pltpu.SemaphoreType.DMA((3, slots)),
        ],
        cost_estimate=pl.CostEstimate(flops=flops, bytes_accessed=moved, transcendentals=0),
        name="tile_products",
    )(meta, *codes, *blocks)


def project_kernel(chan_ref, p0, p1, p2, p3, enc_mix, dec_proj, node_embed, hidden, node_grad):
    chan = chan_ref[0]
    mixed = None
    for back, piece in enumerate((p0, p1, p2, p3)):
        rows = pl.ds(pl.multiple_of(((chan + CHAN - back) % CHAN) * 256, 256), 256)
        left = jnp.dot(piece[0], enc_mix[rows, :], preferred_element_type=jnp.float32)
        right = jnp.dot(piece[1], dec_proj[rows, :], preferred_element_type=jnp.float32)
        mixed, grad = (left, right) if mixed is None else (mixed + left, grad + right)
    hidden[...] = (node_embed[...].astype(jnp.float32) + mixed / (1.0 + jnp.exp(-mixed))).astype(hidden.dtype)
    node_grad[...] = grad.astype(node_grad.dtype)


def project(chan, pieces, enc_mix, dec_proj, node_embed):
    rows, channels = node_embed.shape
    vmem = pl.BlockSpec(memory_space=pltpu.VMEM)
    return pl.pallas_call(
        project_kernel,
        out_shape=[jax.ShapeDtypeStruct((rows, channels), jnp.bfloat16)] * 2,
        in_specs=[pl.BlockSpec(memory_space=pltpu.SMEM)] + [vmem] * 7,
        out_specs=[vmem] * 2,
        cost_estimate=pl.CostEstimate(
            flops=4 * rows * CHAN * channels * channels,
            bytes_accessed=4 * CHAN * rows * channels * 4,
            transcendentals=rows * channels,
        ),
        name="project",
    )(chan.reshape(1), *pieces, enc_mix, dec_proj, node_embed)


def near_step(band):
    return 1 - 2 * (band // 2 % 2)


def one_device(
    cells_next, node_embed, enc_mix, out_cotangent, decoded_saved, dec_proj, tile_source, tile_codes
):
    bands = lax.axis_size("band")
    band = lax.axis_index("band")
    chan = lax.axis_index("chan")
    core = band % 2
    tile_scale = (3.0 / (K * BLK)) ** 0.5 / 128.0
    channels = cells_next.shape[1]
    go = functools.partial(permute, bands=bands)
    codes = tile_codes.reshape(TILES, BLK, BLK)
    cells = cells_next.reshape(CB_DEV, BLK, channels)
    cotangent = out_cotangent.reshape(CB_DEV, BLK, channels)
    quarter = SIDE // CHAN

    cells_sib = go(cells, lambda b, c: (b ^ 1, c))
    cotangent_sib = go(cotangent, lambda b, c: (b ^ 1, c))

    place = jnp.stack([band, chan]).astype(jnp.int32)
    give_codes, keep_codes = pick_tiles(place, tile_source.T, codes, ((0, "mirrored"), (1, "mirrored")))
    give_extra, keep_extra, far_codes = pick_tiles(place, tile_source.T, codes, ((0, "own"), (1, "own"), (2, "all")))
    ends = (0, CHAN - 1)

    def mirrored(c):
        return CHAN - 1 - c

    def if_end(c):
        return mirrored(c) if c in ends else -1

    give_codes = go(give_codes, lambda b, c: (b - 2 * near_step(b), mirrored(c)))
    keep_codes = go(keep_codes, lambda b, c: (b ^ 2, mirrored(c)))
    give_extra = go(give_extra, lambda b, c: (b - 2 * near_step(b), if_end(c)))
    keep_extra = go(keep_extra, lambda b, c: (b ^ 2, if_end(c)))
    far_codes = go(far_codes, lambda b, c: (b - 2 * far_step(b), c))

    def along_chan(x, extra):
        return [x] + [go(x, lambda b, c, by=by: (b, c + by)) for by in (1, -1, 2, -2)] + [extra]

    give_codes = along_chan(give_codes, give_extra)
    keep_codes = along_chan(keep_codes, keep_extra)

    def over_chan(x):
        return [x] + [go(x, lambda b, c, by=by: (b, (c + by) % CHAN)) for by in range(1, CHAN)]

    half = decoded_saved.shape[0] // 2
    dec_first = go(decoded_saved[:half], lambda b, c: (b, c ^ 2))
    cot_pair = go(out_cotangent, lambda b, c: (b, c ^ 1))
    dec_second = go(decoded_saved[half:], lambda b, c: (b, c ^ 2))

    near = near_step(band)
    far = far_step_traced(core)
    readers = band + jnp.array([2, -2, 0, 0], jnp.int32) * near + jnp.array([0, 0, 2, 0], jnp.int32) * far
    offsets = jnp.array([-1, 1, 0, 0], jnp.int32) * near + jnp.array([0, 0, -1, 0], jnp.int32) * far
    tile, block = slot_table(tile_source, readers, offsets)

    slots = jnp.arange(SIDE, dtype=jnp.int32)

    def meta_of(row, index):
        node = jnp.where(tile[row] < 0, NB_DEV, tile[row] // K)
        own = (block[row] // CB_DEV == core).astype(jnp.int32)
        away = slots // quarter - chan
        operand = jnp.where(away < 0, -2 * away - 1, 2 * away)
        operand = jnp.where(jnp.abs(away) == CHAN - 1, 5, operand)
        return jnp.stack([node, own, block[row] % CB_DEV, index, operand])

    def pieces_meta(row):
        return meta_of(row, slots % quarter)

    blocks = (cells, cells_sib, cotangent, cotangent_sib)
    piece_group = [[(tuple(range(6)), 0, SIDE)]]
    near_meta = jnp.concatenate([meta_of(2, slots)[:, :CAP], meta_of(3, jnp.maximum(tile[3], 0))], axis=1)
    far_part, own_part = tile_products(
        near_meta, [far_codes, codes], blocks, [[((0,), 0, CAP)], [((1,), CAP, SIDE)]], [jnp.bfloat16, jnp.float32]
    )
    got_far = go(far_part, lambda b, c: (b + 2 * far_step(b), c))
    (give_part,) = tile_products(pieces_meta(1), give_codes, blocks, piece_group, [jnp.bfloat16])
    got_give = go(give_part, lambda b, c: (b - 4 * near_step(b), c))
    (keep_part,) = tile_products(pieces_meta(0), keep_codes, blocks, piece_group, [jnp.float32])
    crossing = (keep_part + got_give.astype(jnp.float32)).astype(jnp.bfloat16)
    got_keep = go(crossing, lambda b, c: (b ^ 2, c))
    summed = own_part + got_keep.astype(jnp.float32) + got_far.astype(jnp.float32)
    aggregates = (summed * tile_scale).astype(jnp.bfloat16)
    pieces = over_chan(aggregates)
    hidden_nodes, node_grad = project(chan, pieces, enc_mix, dec_proj, node_embed)

    w_dec_grad = projection_gradient(go, out_cotangent, decoded_saved, cot_pair, (dec_first, dec_second), bands)
    return (hidden_nodes, node_grad, w_dec_grad)


def far_step_traced(core):
    return 2 - 4 * core


def projection_gradient(go, cot, dec, cot_pair, dec_pair, bands):
    band, chan = lax.axis_index("band"), lax.axis_index("chan")
    along = bands // 16
    x, y, zh, core = band // (4 * along), band // along % 4, band // 2 % 2, band % 2
    channels = cot.shape[1]
    cells_total = cot.shape[0] * bands
    rows = channels // 16

    def outer(left, right):
        return lax.dot_general(left, right, (((0,), (0,)), ((), ())), preferred_element_type=jnp.float32)

    half = cot.shape[0] // 2
    first = outer(cot, dec)
    third = lax.optimization_barrier(outer(cot[:half], dec_pair[0]))
    second = outer(cot_pair, dec)
    third = third + outer(cot[half:], dec_pair[1])
    fourth = outer(cot_pair[:half], dec_pair[0]) + outer(cot_pair[half:], dec_pair[1])
    whole = jnp.stack([first, second, third, fourth])
    halves = whole.reshape(4, 8, 2, rows, channels)
    own = lax.dynamic_index_in_dim(halves, core, 2, keepdims=False)
    other = lax.dynamic_index_in_dim(halves, 1 - core, 2, keepdims=False).astype(jnp.bfloat16)
    own = own + go(other, lambda b, c: (b ^ 1, c)).astype(jnp.float32)

    def take(i):
        return lax.dynamic_index_in_dim(own, i, 0, keepdims=False)

    share = take(x ^ chan)
    for by in range(1, 4):
        sent = take(((x + by) % 4) ^ chan).astype(jnp.bfloat16)
        share = share + go(sent, lambda b, c: ((b + by * 4 * along) % bands, c)).astype(jnp.float32)

    own = share.reshape(4, 2, rows, channels)
    share = take(y)
    for by in range(1, 4):
        sent = take((y + by) % 4)
        share = share + go(sent, lambda b, c: (b // 16 * 16 + (b % 16 + by * 4) % 16, c))

    def home(b, c):
        at_x, rest = b // 16, b % 16
        return (2 * (c // 2) + at_x % 2) * 16 + rest, c % 2 + 2 * (at_x // 2)

    def home_across(b, c):
        return home(b ^ 2, c)

    own = share
    return (go(take(zh), home) + go(take(1 - zh), home_across)) * cells_total ** (-0.5)


def solution(mesh):
    in_specs = (
        P("band", "chan"),
        P("band", "chan"),
        P(None, "chan"),
        P("band", "chan"),
        P("band", "chan"),
        P(None, "chan"),
        P(),
        P("band", None, None, None),
    )
    out_specs = (P("band", "chan"), P("band", "chan"), P("band", "chan"))
    return jax.shard_map(one_device, mesh=mesh, in_specs=in_specs, out_specs=out_specs, check_vma=False)
```

```python
import functools

import jax
import jax.numpy as jnp
from jax import lax
from jax.experimental import pallas as pl
from jax.experimental.pallas import tpu as pltpu
from jax.sharding import PartitionSpec as P


BLK = 128
K = 16
CB_DEV = 16
NB_DEV = 2
CAP = 8
CHAN = 4
TILES = NB_DEV * K
PAIR_BLOCKS = 2 * CB_DEV
SIDE = 2 * CAP


def permute(x, move, bands):
    pairs = []
    for band in range(bands):
        for chan in range(CHAN):
            to_band, to_chan = move(band, chan)
            if 0 <= to_band < bands and 0 <= to_chan < CHAN:
                pairs.append((band * CHAN + chan, to_band * CHAN + to_chan))
    return lax.ppermute(x, ("band", "chan"), pairs)


def far_step(band):
    return 2 if band % 2 == 0 else -2


def slot_table(tile_source, readers, offsets):
    bands = tile_source.shape[0] // NB_DEV
    rows = tile_source.reshape(bands, TILES)[jnp.clip(readers, 0, bands - 1)]
    hit = (rows // PAIR_BLOCKS - (readers // 2)[:, None]) == offsets[:, None]
    earlier = jnp.tril(jnp.ones((TILES, TILES), jnp.int32), -1)
    rank = jnp.sum(hit.astype(jnp.int32)[:, None, :] * earlier[None], axis=2)
    code = (jnp.arange(TILES, dtype=jnp.int32) * PAIR_BLOCKS)[None] + rows % PAIR_BLOCKS + 1
    chosen = hit[:, None, :] & (rank[:, None, :] == jnp.arange(SIDE, dtype=jnp.int32)[None, :, None])
    packed = jnp.sum(jnp.where(chosen, code[:, None, :], 0), axis=2) - 1
    tile = jnp.where(packed < 0, -1, packed // PAIR_BLOCKS)
    block = jnp.where(packed < 0, 0, packed % PAIR_BLOCKS)
    return tile, block


def pick_kernel(picks, place, rows, codes, *refs):
    outs, (listed, sems) = refs[:-2], refs[-2:]
    band, chan = place[0], place[1]
    chip = band // 2
    near = 1 - 2 * (chip % 2)
    far = 2 - 4 * (band % 2)
    starts = {"mirrored": (CHAN - 1 - chan) * (SIDE // CHAN), "own": chan * (SIDE // CHAN), "all": 0}
    for i in range(3 * SIDE):
        listed[i] = 0

    def sort(tile, counts):
        offset = rows[tile % K, band * NB_DEV + tile // K] // PAIR_BLOCKS - chip
        after = []
        for kind, (wanted, count) in enumerate(zip((-near, near, -far), counts)):
            hit = offset == wanted

            @pl.when(hit & (count < SIDE))
            def _(kind=kind, count=count):
                listed[kind * SIDE + count] = tile

            after.append(count + hit.astype(jnp.int32))
        return tuple(after)

    zero = jnp.int32(0)
    lax.fori_loop(0, TILES, sort, (zero, zero, zero))
    copies = []
    for out, (kind, which) in zip(outs, picks):
        for i in range(out.shape[0]):
            tile = listed[kind * SIDE + starts[which] + i]
            copies.append(pltpu.make_async_copy(codes.at[tile], out.at[i], sems.at[len(copies)]))
            copies[-1].start()
    for copy in copies:
        copy.wait()


def pick_tiles(place, rows, codes, picks):
    counts = [CAP if which == "all" else SIDE // CHAN for _, which in picks]
    smem = pl.BlockSpec(memory_space=pltpu.SMEM)
    return pl.pallas_call(
        functools.partial(pick_kernel, picks),
        out_shape=[jax.ShapeDtypeStruct((count, BLK, BLK), codes.dtype) for count in counts],
        in_specs=[smem, smem, pl.BlockSpec(memory_space=pl.ANY)],
        out_specs=[pl.BlockSpec(memory_space=pltpu.VMEM)] * len(counts),
        scratch_shapes=[pltpu.SMEM((3 * SIDE,), jnp.int32), pltpu.SemaphoreType.DMA((sum(counts),))],
        cost_estimate=pl.CostEstimate(flops=10**8, bytes_accessed=2 * sum(counts) * BLK * BLK * 4, transcendentals=0),
        name="pick_tiles",
    )(place, rows, codes)


def products_kernel(groups, n_codes, *refs):
    meta = refs[0]
    codes = refs[1 : 1 + n_codes]
    cells_own, cells_sib, cot_own, cot_sib = refs[1 + n_codes : 5 + n_codes]
    outs = refs[5 + n_codes : 5 + n_codes + len(groups)]
    code_buf, cell_buf, cot_buf, total, sems = refs[5 + n_codes + len(groups) :]
    for parts in groups:
        for operands, first, count in parts:

            def begin(i, carry, first=first, operands=operands):
                slot = first + i
                for operand in operands:

                    @pl.when((meta[4, slot] == operand) | (len(operands) == 1))
                    def _(operand=operand):
                        pltpu.make_async_copy(
                            codes[operand].at[meta[3, slot]], code_buf.at[slot], sems.at[0, slot]
                        ).start()

                local = meta[2, slot]

                @pl.when(meta[1, slot] == 1)
                def _():
                    pltpu.make_async_copy(cells_own.at[local], cell_buf.at[slot], sems.at[1, slot]).start()
                    pltpu.make_async_copy(cot_own.at[local], cot_buf.at[slot], sems.at[2, slot]).start()

                @pl.when(meta[1, slot] != 1)
                def _():
                    pltpu.make_async_copy(cells_sib.at[local], cell_buf.at[slot], sems.at[1, slot]).start()
                    pltpu.make_async_copy(cot_sib.at[local], cot_buf.at[slot], sems.at[2, slot]).start()

                return carry

            lax.fori_loop(0, count, begin, 0)

    for out, parts in zip(outs, groups):
        total[...] = jnp.zeros_like(total)
        first = parts[0][1]
        slots = sum(count for _, _, count in parts)

        def step(i, carry, first=first):
            enc_rows, dec_rows = [[], []], [[], []]
            base = first + i * 4
            for inner in range(4):
                slot = base + inner
                pltpu.make_async_copy(codes[0].at[0], code_buf.at[slot], sems.at[0, slot]).wait()
                pltpu.make_async_copy(cells_own.at[0], cell_buf.at[slot], sems.at[1, slot]).wait()
                pltpu.make_async_copy(cot_own.at[0], cot_buf.at[slot], sems.at[2, slot]).wait()
                words = code_buf[slot]
                enc = ((words & 255) - 128).astype(jnp.float32)
                dec = ((words >> 8) - 128).astype(jnp.float32)
                for node in range(NB_DEV):
                    keep = (meta[0, slot] == node).astype(jnp.float32)
                    enc_rows[node].append((enc * keep).astype(jnp.bfloat16))
                    dec_rows[node].append((dec * keep).astype(jnp.bfloat16))
            wide = [
                jnp.concatenate([jnp.concatenate(line, axis=1) for line in both], axis=0)
                for both in (enc_rows, dec_rows)
            ]
            cells = cell_buf[pl.ds(base, 4)].reshape(4 * BLK, -1)
            cots = cot_buf[pl.ds(base, 4)].reshape(4 * BLK, -1)
            total[0] += jnp.dot(wide[0], cells, preferred_element_type=jnp.float32)
            total[1] += jnp.dot(wide[1], cots, preferred_element_type=jnp.float32)
            return carry

        lax.fori_loop(0, slots // 4, step, 0)
        out[...] = total[...].astype(out.dtype)


def tile_products(meta, codes, blocks, groups, dtypes):
    slots = meta.shape[1]
    channels = blocks[0].shape[-1]
    flops = slots * 4 * BLK * BLK * channels
    moved = slots * (BLK * BLK * 4 + 2 * BLK * channels * 2)
    return pl.pallas_call(
        functools.partial(products_kernel, groups, len(codes)),
        out_shape=[jax.ShapeDtypeStruct((2, NB_DEV * BLK, channels), dtype) for dtype in dtypes],
        in_specs=[pl.BlockSpec(memory_space=pltpu.SMEM)]
        + [pl.BlockSpec(memory_space=pl.ANY)] * (len(codes) + 4),
        out_specs=[pl.BlockSpec(memory_space=pltpu.VMEM)] * len(dtypes),
        scratch_shapes=[
            pltpu.VMEM((slots, BLK, BLK), jnp.int32),
            pltpu.VMEM((slots, BLK, channels), jnp.bfloat16),
            pltpu.VMEM((slots, BLK, channels), jnp.bfloat16),
            pltpu.VMEM((2, NB_DEV * BLK, channels), jnp.float32),
            pltpu.SemaphoreType.DMA((3, slots)),
        ],
        cost_estimate=pl.CostEstimate(flops=flops, bytes_accessed=moved, transcendentals=0),
        name="tile_products",
    )(meta, *codes, *blocks)


def project_kernel(chan_ref, p0, p1, p2, p3, enc_mix, dec_proj, node_embed, hidden, node_grad):
    chan = chan_ref[0]
    mixed = None
    for by, piece in enumerate((p0, p1, p2, p3)):
        rows = pl.ds(pl.multiple_of((chan ^ by) * 256, 256), 256)
        left = jnp.dot(piece[0], enc_mix[rows, :], preferred_element_type=jnp.float32)
        right = jnp.dot(piece[1], dec_proj[rows, :], preferred_element_type=jnp.float32)
        mixed, grad = (left, right) if mixed is None else (mixed + left, grad + right)
    hidden[...] = (node_embed[...].astype(jnp.float32) + mixed / (1.0 + jnp.exp(-mixed))).astype(hidden.dtype)
    node_grad[...] = grad.astype(node_grad.dtype)


def project(chan, pieces, enc_mix, dec_proj, node_embed):
    rows, channels = node_embed.shape
    vmem = pl.BlockSpec(memory_space=pltpu.VMEM)
    return pl.pallas_call(
        project_kernel,
        out_shape=[jax.ShapeDtypeStruct((rows, channels), jnp.bfloat16)] * 2,
        in_specs=[pl.BlockSpec(memory_space=pltpu.SMEM)] + [vmem] * 7,
        out_specs=[vmem] * 2,
        cost_estimate=pl.CostEstimate(
            flops=4 * rows * CHAN * channels * channels,
            bytes_accessed=4 * CHAN * rows * channels * 4,
            transcendentals=rows * channels,
        ),
        name="project",
    )(chan.reshape(1), *pieces, enc_mix, dec_proj, node_embed)


def near_step(band):
    return 1 - 2 * (band // 2 % 2)


def one_device(
    cells_next, node_embed, enc_mix, out_cotangent, decoded_saved, dec_proj, tile_source, tile_codes
):
    bands = lax.axis_size("band")
    band = lax.axis_index("band")
    chan = lax.axis_index("chan")
    core = band % 2
    tile_scale = (3.0 / (K * BLK)) ** 0.5 / 128.0
    channels = cells_next.shape[1]
    go = functools.partial(permute, bands=bands)
    codes = tile_codes.reshape(TILES, BLK, BLK)
    cells = cells_next.reshape(CB_DEV, BLK, channels)
    cotangent = out_cotangent.reshape(CB_DEV, BLK, channels)
    quarter = SIDE // CHAN

    cells_sib = go(cells, lambda b, c: (b ^ 1, c))
    cotangent_sib = go(cotangent, lambda b, c: (b ^ 1, c))

    place = jnp.stack([band, chan]).astype(jnp.int32)
    give_codes, keep_codes = pick_tiles(place, tile_source.T, codes, ((0, "mirrored"), (1, "mirrored")))
    give_extra, keep_extra, far_codes = pick_tiles(place, tile_source.T, codes, ((0, "own"), (1, "own"), (2, "all")))

    def mirrored(c):
        return CHAN - 1 - c

    give_to = lambda b: b - 2 * near_step(b)
    keep_to = lambda b: b ^ 2

    give_codes = go(give_codes, lambda b, c: (give_to(b), mirrored(c)))
    keep_codes = go(keep_codes, lambda b, c: (keep_to(b), mirrored(c)))
    far_codes = go(far_codes, lambda b, c: (b - 2 * far_step(b), c))

    at_end = (chan == 0) | (chan == CHAN - 1)

    def along_chan(x, extra, reader):
        one, two = (go(x, lambda b, c, by=by: (b, c ^ by)) for by in (1, 2))
        three = go(
            jnp.where(at_end, extra, x),
            lambda b, c: (reader(b) if c in (0, CHAN - 1) else b, mirrored(c)),
        )
        return [x, one, two, three]

    give_codes = along_chan(give_codes, give_extra, give_to)
    keep_codes = along_chan(keep_codes, keep_extra, keep_to)

    def over_chan(x):
        return [x] + [go(x, lambda b, c, by=by: (b, c ^ by)) for by in range(1, CHAN)]

    half = decoded_saved.shape[0] // 2
    dec_first = go(decoded_saved[:half], lambda b, c: (b, c ^ 2))
    cot_pair = go(out_cotangent, lambda b, c: (b, c ^ 1))
    dec_second = go(decoded_saved[half:], lambda b, c: (b, c ^ 2))

    near = near_step(band)
    far = far_step_traced(core)
    readers = band + jnp.array([2, -2, 0, 0], jnp.int32) * near + jnp.array([0, 0, 2, 0], jnp.int32) * far
    offsets = jnp.array([-1, 1, 0, 0], jnp.int32) * near + jnp.array([0, 0, -1, 0], jnp.int32) * far
    tile, block = slot_table(tile_source, readers, offsets)

    slots = jnp.arange(SIDE, dtype=jnp.int32)

    def meta_of(row, index):
        node = jnp.where(tile[row] < 0, NB_DEV, tile[row] // K)
        own = (block[row] // CB_DEV == core).astype(jnp.int32)
        return jnp.stack([node, own, block[row] % CB_DEV, index, (slots // quarter) ^ chan])

    def pieces_meta(row):
        return meta_of(row, slots % quarter)

    blocks = (cells, cells_sib, cotangent, cotangent_sib)
    piece_group = [[(tuple(range(CHAN)), 0, SIDE)]]
    near_meta = jnp.concatenate([meta_of(2, slots)[:, :CAP], meta_of(3, jnp.maximum(tile[3], 0))], axis=1)
    far_part, own_part = tile_products(
        near_meta, [far_codes, codes], blocks, [[((0,), 0, CAP)], [((1,), CAP, SIDE)]], [jnp.bfloat16, jnp.float32]
    )
    got_far = go(far_part, lambda b, c: (b + 2 * far_step(b), c))
    (give_part,) = tile_products(pieces_meta(1), give_codes, blocks, piece_group, [jnp.bfloat16])
    got_give = go(give_part, lambda b, c: (b - 4 * near_step(b), c))
    (keep_part,) = tile_products(pieces_meta(0), keep_codes, blocks, piece_group, [jnp.float32])
    crossing = (keep_part + got_give.astype(jnp.float32)).astype(jnp.bfloat16)
    got_keep = go(crossing, lambda b, c: (b ^ 2, c))
    summed = own_part + got_keep.astype(jnp.float32) + got_far.astype(jnp.float32)
    aggregates = (summed * tile_scale).astype(jnp.bfloat16)
    pieces = over_chan(aggregates)
    hidden_nodes, node_grad = project(chan, pieces, enc_mix, dec_proj, node_embed)

    w_dec_grad = projection_gradient(go, out_cotangent, decoded_saved, cot_pair, (dec_first, dec_second), bands)
    return (hidden_nodes, node_grad, w_dec_grad)


def far_step_traced(core):
    return 2 - 4 * core


def projection_gradient(go, cot, dec, cot_pair, dec_pair, bands):
    band, chan = lax.axis_index("band"), lax.axis_index("chan")
    along = bands // 16
    x, y, zh, core = band // (4 * along), band // along % 4, band // 2 % 2, band % 2
    channels = cot.shape[1]
    cells_total = cot.shape[0] * bands
    rows = channels // 16

    def outer(left, right):
        return lax.dot_general(left, right, (((0,), (0,)), ((), ())), preferred_element_type=jnp.float32)

    half = cot.shape[0] // 2
    first = outer(cot, dec)
    third = lax.optimization_barrier(outer(cot[:half], dec_pair[0]))
    second = outer(cot_pair, dec)
    fourth = lax.optimization_barrier(outer(cot_pair[:half], dec_pair[0]))
    third = third + outer(cot[half:], dec_pair[1])
    fourth = fourth + outer(cot_pair[half:], dec_pair[1])
    whole = jnp.stack([first, second, third, fourth])
    halves = whole.reshape(4, 8, 2, rows, channels)
    own = lax.dynamic_index_in_dim(halves, core, 2, keepdims=False)
    other = lax.dynamic_index_in_dim(halves, 1 - core, 2, keepdims=False).astype(jnp.bfloat16)
    own = own + go(other, lambda b, c: (b ^ 1, c)).astype(jnp.float32)

    def take(i):
        return lax.dynamic_index_in_dim(own, i, 0, keepdims=False)

    share = take(x ^ chan)
    for by in range(1, 4):
        sent = take(x ^ by ^ chan).astype(jnp.bfloat16)
        share = share + go(sent, lambda b, c: (b ^ (by * 4 * along), c)).astype(jnp.float32)

    own = share.reshape(4, 2, rows, channels)
    share = take(y)
    for by in range(1, 4):
        share = share + go(take(y ^ by), lambda b, c: (b ^ (by * 4), c))

    def home(b, c):
        at_x, rest = b // 16, b % 16
        return (2 * (c // 2) + at_x % 2) * 16 + rest, c % 2 + 2 * (at_x // 2)

    def home_across(b, c):
        return home(b ^ 2, c)

    own = share
    return (go(take(zh), home) + go(take(1 - zh), home_across)) * cells_total ** (-0.5)


def solution(mesh):
    in_specs = (
        P("band", "chan"),
        P("band", "chan"),
        P(None, "chan"),
        P("band", "chan"),
        P("band", "chan"),
        P(None, "chan"),
        P(),
        P("band", None, None, None),
    )
    out_specs = (P("band", "chan"), P("band", "chan"), P("band", "chan"))
    return jax.shard_map(one_device, mesh=mesh, in_specs=in_specs, out_specs=out_specs, check_vma=False)
```

```python
import functools

import jax
import jax.numpy as jnp
from jax import lax
from jax.experimental import pallas as pl
from jax.experimental.pallas import tpu as pltpu
from jax.sharding import PartitionSpec as P


BLK = 128
K = 16
CB_DEV = 16
NB_DEV = 2
CAP = 8
CHAN = 4
TILES = NB_DEV * K
PAIR_BLOCKS = 2 * CB_DEV
SIDE = 2 * CAP
VMEM_GRANT = 12 * 2**20


def permute(x, move, bands):
    pairs = []
    for band in range(bands):
        for chan in range(CHAN):
            to_band, to_chan = move(band, chan)
            if 0 <= to_band < bands and 0 <= to_chan < CHAN:
                pairs.append((band * CHAN + chan, to_band * CHAN + to_chan))
    return lax.ppermute(x, ("band", "chan"), pairs)


def far_step(band):
    return 2 if band % 2 == 0 else -2


def slot_table(tile_source, readers, offsets):
    bands = tile_source.shape[0] // NB_DEV
    rows = tile_source.reshape(bands, TILES)[jnp.clip(readers, 0, bands - 1)]
    hit = (rows // PAIR_BLOCKS - (readers // 2)[:, None]) == offsets[:, None]
    earlier = jnp.tril(jnp.ones((TILES, TILES), jnp.int32), -1)
    rank = jnp.sum(hit.astype(jnp.int32)[:, None, :] * earlier[None], axis=2)
    code = (jnp.arange(TILES, dtype=jnp.int32) * PAIR_BLOCKS)[None] + rows % PAIR_BLOCKS + 1
    chosen = hit[:, None, :] & (rank[:, None, :] == jnp.arange(SIDE, dtype=jnp.int32)[None, :, None])
    packed = jnp.sum(jnp.where(chosen, code[:, None, :], 0), axis=2) - 1
    tile = jnp.where(packed < 0, -1, packed // PAIR_BLOCKS)
    block = jnp.where(packed < 0, 0, packed % PAIR_BLOCKS)
    return tile, block


def pick_kernel(picks, place, rows, codes, *refs):
    outs, (listed, sems) = refs[:-2], refs[-2:]
    band, chan = place[0], place[1]
    chip = band // 2
    near = 1 - 2 * (chip % 2)
    far = 2 - 4 * (band % 2)
    starts = {"mirrored": (CHAN - 1 - chan) * (SIDE // CHAN), "own": chan * (SIDE // CHAN), "all": 0}
    for i in range(3 * SIDE):
        listed[i] = 0

    def sort(tile, counts):
        offset = rows[tile % K, band * NB_DEV + tile // K] // PAIR_BLOCKS - chip
        after = []
        for kind, (wanted, count) in enumerate(zip((-near, near, -far), counts)):
            hit = offset == wanted

            @pl.when(hit & (count < SIDE))
            def _(kind=kind, count=count):
                listed[kind * SIDE + count] = tile

            after.append(count + hit.astype(jnp.int32))
        return tuple(after)

    zero = jnp.int32(0)
    lax.fori_loop(0, TILES, sort, (zero, zero, zero))
    copies = []
    for out, (kind, which) in zip(outs, picks):
        for i in range(out.shape[0]):
            tile = listed[kind * SIDE + starts[which] + i]
            copies.append(pltpu.make_async_copy(codes.at[tile], out.at[i], sems.at[len(copies)]))
            copies[-1].start()
    for copy in copies:
        copy.wait()


def pick_tiles(place, rows, codes, picks):
    counts = [CAP if which == "all" else SIDE // CHAN for _, which in picks]
    smem = pl.BlockSpec(memory_space=pltpu.SMEM)
    return pl.pallas_call(
        functools.partial(pick_kernel, picks),
        out_shape=[jax.ShapeDtypeStruct((count, BLK, BLK), codes.dtype) for count in counts],
        in_specs=[smem, smem, pl.BlockSpec(memory_space=pl.ANY)],
        out_specs=[pl.BlockSpec(memory_space=pltpu.VMEM)] * len(counts),
        scratch_shapes=[pltpu.SMEM((3 * SIDE,), jnp.int32), pltpu.SemaphoreType.DMA((sum(counts),))],
        cost_estimate=pl.CostEstimate(flops=10**8, bytes_accessed=2 * sum(counts) * BLK * BLK * 4, transcendentals=0),
        compiler_params=pltpu.CompilerParams(vmem_limit_bytes=VMEM_GRANT),
        name="pick_tiles",
    )(place, rows, codes)


def products_kernel(groups, n_codes, *refs):
    meta = refs[0]
    codes = refs[1 : 1 + n_codes]
    cells_own, cells_sib, cot_own, cot_sib = refs[1 + n_codes : 5 + n_codes]
    outs = refs[5 + n_codes : 5 + n_codes + len(groups)]
    code_buf, cell_buf, cot_buf, total, sems = refs[5 + n_codes + len(groups) :]
    for parts in groups:
        for operands, first, count in parts:

            def begin(i, carry, first=first, operands=operands):
                slot = first + i
                for operand in operands:

                    @pl.when((meta[4, slot] == operand) | (len(operands) == 1))
                    def _(operand=operand):
                        pltpu.make_async_copy(
                            codes[operand].at[meta[3, slot]], code_buf.at[slot], sems.at[0, slot]
                        ).start()

                local = meta[2, slot]

                @pl.when(meta[1, slot] == 1)
                def _():
                    pltpu.make_async_copy(cells_own.at[local], cell_buf.at[slot], sems.at[1, slot]).start()
                    pltpu.make_async_copy(cot_own.at[local], cot_buf.at[slot], sems.at[2, slot]).start()

                @pl.when(meta[1, slot] != 1)
                def _():
                    pltpu.make_async_copy(cells_sib.at[local], cell_buf.at[slot], sems.at[1, slot]).start()
                    pltpu.make_async_copy(cot_sib.at[local], cot_buf.at[slot], sems.at[2, slot]).start()

                return carry

            lax.fori_loop(0, count, begin, 0)

    for out, parts in zip(outs, groups):
        total[...] = jnp.zeros_like(total)
        first = parts[0][1]
        slots = sum(count for _, _, count in parts)

        def step(i, carry, first=first):
            enc_rows, dec_rows = [[], []], [[], []]
            base = first + i * 4
            for inner in range(4):
                slot = base + inner
                pltpu.make_async_copy(codes[0].at[0], code_buf.at[slot], sems.at[0, slot]).wait()
                pltpu.make_async_copy(cells_own.at[0], cell_buf.at[slot], sems.at[1, slot]).wait()
                pltpu.make_async_copy(cot_own.at[0], cot_buf.at[slot], sems.at[2, slot]).wait()
                words = code_buf[slot]
                enc = ((words & 255) - 128).astype(jnp.float32)
                dec = ((words >> 8) - 128).astype(jnp.float32)
                for node in range(NB_DEV):
                    keep = (meta[0, slot] == node).astype(jnp.float32)
                    enc_rows[node].append((enc * keep).astype(jnp.bfloat16))
                    dec_rows[node].append((dec * keep).astype(jnp.bfloat16))
            wide = [
                jnp.concatenate([jnp.concatenate(line, axis=1) for line in both], axis=0)
                for both in (enc_rows, dec_rows)
            ]
            cells = cell_buf[pl.ds(base, 4)].reshape(4 * BLK, -1)
            cots = cot_buf[pl.ds(base, 4)].reshape(4 * BLK, -1)
            total[0] += jnp.dot(wide[0], cells, preferred_element_type=jnp.float32)
            total[1] += jnp.dot(wide[1], cots, preferred_element_type=jnp.float32)
            return carry

        lax.fori_loop(0, slots // 4, step, 0)
        out[...] = total[...].astype(out.dtype)


def tile_products(meta, codes, blocks, groups, dtypes):
    slots = meta.shape[1]
    channels = blocks[0].shape[-1]
    flops = slots * 4 * BLK * BLK * channels
    moved = slots * (BLK * BLK * 4 + 2 * BLK * channels * 2)
    return pl.pallas_call(
        functools.partial(products_kernel, groups, len(codes)),
        out_shape=[jax.ShapeDtypeStruct((2, NB_DEV * BLK, channels), dtype) for dtype in dtypes],
        in_specs=[pl.BlockSpec(memory_space=pltpu.SMEM)]
        + [pl.BlockSpec(memory_space=pl.ANY)] * (len(codes) + 4),
        out_specs=[pl.BlockSpec(memory_space=pltpu.VMEM)] * len(dtypes),
        scratch_shapes=[
            pltpu.VMEM((slots, BLK, BLK), jnp.int32),
            pltpu.VMEM((slots, BLK, channels), jnp.bfloat16),
            pltpu.VMEM((slots, BLK, channels), jnp.bfloat16),
            pltpu.VMEM((2, NB_DEV * BLK, channels), jnp.float32),
            pltpu.SemaphoreType.DMA((3, slots)),
        ],
        cost_estimate=pl.CostEstimate(flops=flops, bytes_accessed=moved, transcendentals=0),
        compiler_params=pltpu.CompilerParams(vmem_limit_bytes=VMEM_GRANT),
        name="tile_products",
    )(meta, *codes, *blocks)


def project_kernel(chan_ref, p0, p1, p2, p3, enc_mix, dec_proj, node_embed, hidden, node_grad):
    chan = chan_ref[0]
    mixed = None
    for by, piece in enumerate((p0, p1, p2, p3)):
        rows = pl.ds(pl.multiple_of((chan ^ by) * 256, 256), 256)
        left = jnp.dot(piece[0], enc_mix[rows, :], preferred_element_type=jnp.float32)
        right = jnp.dot(piece[1], dec_proj[rows, :], preferred_element_type=jnp.float32)
        mixed, grad = (left, right) if mixed is None else (mixed + left, grad + right)
    hidden[...] = (node_embed[...].astype(jnp.float32) + mixed / (1.0 + jnp.exp(-mixed))).astype(hidden.dtype)
    node_grad[...] = grad.astype(node_grad.dtype)


def project(chan, pieces, enc_mix, dec_proj, node_embed):
    rows, channels = node_embed.shape
    vmem = pl.BlockSpec(memory_space=pltpu.VMEM)
    return pl.pallas_call(
        project_kernel,
        out_shape=[jax.ShapeDtypeStruct((rows, channels), jnp.bfloat16)] * 2,
        in_specs=[pl.BlockSpec(memory_space=pltpu.SMEM)] + [vmem] * 7,
        out_specs=[vmem] * 2,
        cost_estimate=pl.CostEstimate(
            flops=4 * rows * CHAN * channels * channels,
            bytes_accessed=4 * CHAN * rows * channels * 4,
            transcendentals=rows * channels,
        ),
        compiler_params=pltpu.CompilerParams(vmem_limit_bytes=VMEM_GRANT),
        name="project",
    )(chan.reshape(1), *pieces, enc_mix, dec_proj, node_embed)


def near_step(band):
    return 1 - 2 * (band // 2 % 2)


def one_device(
    cells_next, node_embed, enc_mix, out_cotangent, decoded_saved, dec_proj, tile_source, tile_codes
):
    bands = lax.axis_size("band")
    band = lax.axis_index("band")
    chan = lax.axis_index("chan")
    core = band % 2
    tile_scale = (3.0 / (K * BLK)) ** 0.5 / 128.0
    channels = cells_next.shape[1]
    go = functools.partial(permute, bands=bands)
    codes = tile_codes.reshape(TILES, BLK, BLK)
    cells = cells_next.reshape(CB_DEV, BLK, channels)
    cotangent = out_cotangent.reshape(CB_DEV, BLK, channels)
    quarter = SIDE // CHAN

    cells_sib = go(cells, lambda b, c: (b ^ 1, c))
    cotangent_sib = go(cotangent, lambda b, c: (b ^ 1, c))

    place = jnp.stack([band, chan]).astype(jnp.int32)
    give_codes, keep_codes = pick_tiles(place, tile_source.T, codes, ((0, "mirrored"), (1, "mirrored")))
    give_extra, keep_extra, far_codes = pick_tiles(place, tile_source.T, codes, ((0, "own"), (1, "own"), (2, "all")))

    def mirrored(c):
        return CHAN - 1 - c

    give_to = lambda b: b - 2 * near_step(b)
    keep_to = lambda b: b ^ 2

    give_codes = go(give_codes, lambda b, c: (give_to(b), mirrored(c)))
    keep_codes = go(keep_codes, lambda b, c: (keep_to(b), mirrored(c)))
    far_codes = go(far_codes, lambda b, c: (b - 2 * far_step(b), c))

    at_end = (chan == 0) | (chan == CHAN - 1)

    def along_chan(x, extra, reader):
        one, two = (go(x, lambda b, c, by=by: (b, c ^ by)) for by in (1, 2))
        three = go(
            jnp.where(at_end, extra, x),
            lambda b, c: (reader(b) if c in (0, CHAN - 1) else b, mirrored(c)),
        )
        return [x, one, two, three]

    give_codes = along_chan(give_codes, give_extra, give_to)
    keep_codes = along_chan(keep_codes, keep_extra, keep_to)

    def over_chan(x):
        return [x] + [go(x, lambda b, c, by=by: (b, c ^ by)) for by in range(1, CHAN)]

    dec_pair = go(decoded_saved, lambda b, c: (b, c ^ 2))
    cot_pair = go(out_cotangent, lambda b, c: (b, c ^ 1))

    near = near_step(band)
    far = far_step_traced(core)
    readers = band + jnp.array([2, -2, 0, 0], jnp.int32) * near + jnp.array([0, 0, 2, 0], jnp.int32) * far
    offsets = jnp.array([-1, 1, 0, 0], jnp.int32) * near + jnp.array([0, 0, -1, 0], jnp.int32) * far
    tile, block = slot_table(tile_source, readers, offsets)

    slots = jnp.arange(SIDE, dtype=jnp.int32)

    def meta_of(row, index):
        node = jnp.where(tile[row] < 0, NB_DEV, tile[row] // K)
        own = (block[row] // CB_DEV == core).astype(jnp.int32)
        return jnp.stack([node, own, block[row] % CB_DEV, index, (slots // quarter) ^ chan])

    def pieces_meta(row):
        return meta_of(row, slots % quarter)

    blocks = (cells, cells_sib, cotangent, cotangent_sib)
    piece_group = [[(tuple(range(CHAN)), 0, SIDE)]]
    near_meta = jnp.concatenate([meta_of(2, slots)[:, :CAP], meta_of(3, jnp.maximum(tile[3], 0))], axis=1)
    far_part, own_part = tile_products(
        near_meta, [far_codes, codes], blocks, [[((0,), 0, CAP)], [((1,), CAP, SIDE)]], [jnp.bfloat16, jnp.float32]
    )
    got_far = go(far_part, lambda b, c: (b + 2 * far_step(b), c))
    (give_part,) = tile_products(pieces_meta(1), give_codes, blocks, piece_group, [jnp.bfloat16])
    got_give = go(give_part, lambda b, c: (b - 4 * near_step(b), c))
    (keep_part,) = tile_products(pieces_meta(0), keep_codes, blocks, piece_group, [jnp.float32])
    crossing = (keep_part + got_give.astype(jnp.float32)).astype(jnp.bfloat16)
    got_keep = go(crossing, lambda b, c: (b ^ 2, c))
    summed = own_part + got_keep.astype(jnp.float32) + got_far.astype(jnp.float32)
    aggregates = (summed * tile_scale).astype(jnp.bfloat16)
    pieces = over_chan(aggregates)
    hidden_nodes, node_grad = project(chan, pieces, enc_mix, dec_proj, node_embed)

    w_dec_grad = projection_gradient(go, out_cotangent, decoded_saved, cot_pair, dec_pair, bands)
    return (hidden_nodes, node_grad, w_dec_grad)


def far_step_traced(core):
    return 2 - 4 * core


def projection_gradient(go, cot, dec, cot_pair, dec_pair, bands):
    band, chan = lax.axis_index("band"), lax.axis_index("chan")
    along = bands // 16
    x, y, zh, core = band // (4 * along), band // along % 4, band // 2 % 2, band % 2
    channels = cot.shape[1]
    cells_total = cot.shape[0] * bands
    rows = channels // 16

    def outer(left, right):
        return lax.dot_general(left, right, (((0,), (0,)), ((), ())), preferred_element_type=jnp.float32)

    first = outer(cot, dec)
    second, third, fourth = outer(cot_pair, dec), outer(cot, dec_pair), outer(cot_pair, dec_pair)
    whole = jnp.stack([first, second, third, fourth])
    halves = whole.reshape(4, 8, 2, rows, channels)
    own = lax.dynamic_index_in_dim(halves, core, 2, keepdims=False)
    other = lax.dynamic_index_in_dim(halves, 1 - core, 2, keepdims=False).astype(jnp.bfloat16)
    own = own + go(other, lambda b, c: (b ^ 1, c)).astype(jnp.float32)

    def take(i):
        return lax.dynamic_index_in_dim(own, i, 0, keepdims=False)

    share = take(x ^ chan)
    for by in range(1, 4):
        sent = take(x ^ by ^ chan).astype(jnp.bfloat16)
        share = share + go(sent, lambda b, c: (b ^ (by * 4 * along), c)).astype(jnp.float32)

    own = share.reshape(4, 2, rows, channels)
    share = take(y)
    for by in range(1, 4):
        share = share + go(take(y ^ by), lambda b, c: (b ^ (by * 4), c))

    def home(b, c):
        at_x, rest = b // 16, b % 16
        return (2 * (c // 2) + at_x % 2) * 16 + rest, c % 2 + 2 * (at_x // 2)

    def home_across(b, c):
        return home(b ^ 2, c)

    own = share
    return (go(take(zh), home) + go(take(1 - zh), home_across)) * cells_total ** (-0.5)


def solution(mesh):
    in_specs = (
        P("band", "chan"),
        P("band", "chan"),
        P(None, "chan"),
        P("band", "chan"),
        P("band", "chan"),
        P(None, "chan"),
        P(),
        P("band", None, None, None),
    )
    out_specs = (P("band", "chan"), P("band", "chan"), P("band", "chan"))
    return jax.shard_map(one_device, mesh=mesh, in_specs=in_specs, out_specs=out_specs, check_vma=False)
```

```python
import functools

import jax
import jax.numpy as jnp
from jax import lax
from jax.experimental import pallas as pl
from jax.experimental.pallas import tpu as pltpu
from jax.sharding import PartitionSpec as P


BLK = 128
K = 16
CB_DEV = 16
NB_DEV = 2
CAP = 8
CHAN = 4
TILES = NB_DEV * K
PAIR_BLOCKS = 2 * CB_DEV
SIDE = 2 * CAP
VMEM_GRANT = 12 * 2**20


def permute(x, move, bands):
    pairs = []
    for band in range(bands):
        for chan in range(CHAN):
            to_band, to_chan = move(band, chan)
            if 0 <= to_band < bands and 0 <= to_chan < CHAN:
                pairs.append((band * CHAN + chan, to_band * CHAN + to_chan))
    return lax.ppermute(x, ("band", "chan"), pairs)


def far_step(band):
    return 2 if band % 2 == 0 else -2


def slot_table(tile_source, readers, offsets):
    bands = tile_source.shape[0] // NB_DEV
    rows = tile_source.reshape(bands, TILES)[jnp.clip(readers, 0, bands - 1)]
    hit = (rows // PAIR_BLOCKS - (readers // 2)[:, None]) == offsets[:, None]
    earlier = jnp.tril(jnp.ones((TILES, TILES), jnp.int32), -1)
    rank = jnp.sum(hit.astype(jnp.int32)[:, None, :] * earlier[None], axis=2)
    code = (jnp.arange(TILES, dtype=jnp.int32) * PAIR_BLOCKS)[None] + rows % PAIR_BLOCKS + 1
    chosen = hit[:, None, :] & (rank[:, None, :] == jnp.arange(SIDE, dtype=jnp.int32)[None, :, None])
    packed = jnp.sum(jnp.where(chosen, code[:, None, :], 0), axis=2) - 1
    tile = jnp.where(packed < 0, -1, packed // PAIR_BLOCKS)
    block = jnp.where(packed < 0, 0, packed % PAIR_BLOCKS)
    return tile, block


def pick_kernel(picks, place, rows, codes, *refs):
    outs, (listed, sems) = refs[:-2], refs[-2:]
    band, chan = place[0], place[1]
    chip = band // 2
    near = 1 - 2 * (chip % 2)
    far = 2 - 4 * (band % 2)
    starts = {"mirrored": (CHAN - 1 - chan) * (SIDE // CHAN), "own": chan * (SIDE // CHAN), "all": 0}
    for i in range(3 * SIDE):
        listed[i] = 0

    def sort(tile, counts):
        offset = rows[tile % K, band * NB_DEV + tile // K] // PAIR_BLOCKS - chip
        after = []
        for kind, (wanted, count) in enumerate(zip((-near, near, -far), counts)):
            hit = offset == wanted

            @pl.when(hit & (count < SIDE))
            def _(kind=kind, count=count):
                listed[kind * SIDE + count] = tile

            after.append(count + hit.astype(jnp.int32))
        return tuple(after)

    zero = jnp.int32(0)
    lax.fori_loop(0, TILES, sort, (zero, zero, zero))
    copies = []
    for out, (kind, which) in zip(outs, picks):
        for i in range(out.shape[0]):
            tile = listed[kind * SIDE + starts[which] + i]
            copies.append(pltpu.make_async_copy(codes.at[tile], out.at[i], sems.at[len(copies)]))
            copies[-1].start()
    for copy in copies:
        copy.wait()


def pick_tiles(place, rows, codes, picks):
    counts = [CAP if which == "all" else SIDE // CHAN for _, which in picks]
    smem = pl.BlockSpec(memory_space=pltpu.SMEM)
    return pl.pallas_call(
        functools.partial(pick_kernel, picks),
        out_shape=[jax.ShapeDtypeStruct((count, BLK, BLK), codes.dtype) for count in counts],
        in_specs=[smem, smem, pl.BlockSpec(memory_space=pl.ANY)],
        out_specs=[pl.BlockSpec(memory_space=pltpu.VMEM)] * len(counts),
        scratch_shapes=[pltpu.SMEM((3 * SIDE,), jnp.int32), pltpu.SemaphoreType.DMA((sum(counts),))],
        cost_estimate=pl.CostEstimate(flops=10**8, bytes_accessed=2 * sum(counts) * BLK * BLK * 4, transcendentals=0),
        compiler_params=pltpu.CompilerParams(vmem_limit_bytes=VMEM_GRANT),
        name="pick_tiles",
    )(place, rows, codes)


def products_kernel(groups, n_codes, *refs):
    meta = refs[0]
    codes = refs[1 : 1 + n_codes]
    cells_own, cells_sib, cot_own, cot_sib = refs[1 + n_codes : 5 + n_codes]
    outs = refs[5 + n_codes : 5 + n_codes + len(groups)]
    code_buf, cell_buf, cot_buf, total, sems = refs[5 + n_codes + len(groups) :]
    for parts in groups:
        for operands, first, count in parts:

            def begin(i, carry, first=first, operands=operands):
                slot = first + i
                for operand in operands:

                    @pl.when((meta[4, slot] == operand) | (len(operands) == 1))
                    def _(operand=operand):
                        pltpu.make_async_copy(
                            codes[operand].at[meta[3, slot]], code_buf.at[slot], sems.at[0, slot]
                        ).start()

                local = meta[2, slot]

                @pl.when(meta[1, slot] == 1)
                def _():
                    pltpu.make_async_copy(cells_own.at[local], cell_buf.at[slot], sems.at[1, slot]).start()
                    pltpu.make_async_copy(cot_own.at[local], cot_buf.at[slot], sems.at[2, slot]).start()

                @pl.when(meta[1, slot] != 1)
                def _():
                    pltpu.make_async_copy(cells_sib.at[local], cell_buf.at[slot], sems.at[1, slot]).start()
                    pltpu.make_async_copy(cot_sib.at[local], cot_buf.at[slot], sems.at[2, slot]).start()

                return carry

            lax.fori_loop(0, count, begin, 0)

    for out, parts in zip(outs, groups):
        total[...] = jnp.zeros_like(total)
        first = parts[0][1]
        slots = sum(count for _, _, count in parts)

        def step(i, carry, first=first):
            enc_rows, dec_rows = [[], []], [[], []]
            base = first + i * 4
            for inner in range(4):
                slot = base + inner
                pltpu.make_async_copy(codes[0].at[0], code_buf.at[slot], sems.at[0, slot]).wait()
                pltpu.make_async_copy(cells_own.at[0], cell_buf.at[slot], sems.at[1, slot]).wait()
                pltpu.make_async_copy(cot_own.at[0], cot_buf.at[slot], sems.at[2, slot]).wait()
                words = code_buf[slot]
                enc = ((words & 255) - 128).astype(jnp.float32)
                dec = ((words >> 8) - 128).astype(jnp.float32)
                for node in range(NB_DEV):
                    keep = (meta[0, slot] == node).astype(jnp.float32)
                    enc_rows[node].append((enc * keep).astype(jnp.bfloat16))
                    dec_rows[node].append((dec * keep).astype(jnp.bfloat16))
            wide = [
                jnp.concatenate([jnp.concatenate(line, axis=1) for line in both], axis=0)
                for both in (enc_rows, dec_rows)
            ]
            cells = cell_buf[pl.ds(base, 4)].reshape(4 * BLK, -1)
            cots = cot_buf[pl.ds(base, 4)].reshape(4 * BLK, -1)
            total[0] += jnp.dot(wide[0], cells, preferred_element_type=jnp.float32)
            total[1] += jnp.dot(wide[1], cots, preferred_element_type=jnp.float32)
            return carry

        lax.fori_loop(0, slots // 4, step, 0)
        out[...] = total[...].astype(out.dtype)


def tile_products(meta, codes, blocks, groups, dtypes):
    slots = meta.shape[1]
    channels = blocks[0].shape[-1]
    flops = slots * 4 * BLK * BLK * channels
    moved = slots * (BLK * BLK * 4 + 2 * BLK * channels * 2)
    return pl.pallas_call(
        functools.partial(products_kernel, groups, len(codes)),
        out_shape=[jax.ShapeDtypeStruct((2, NB_DEV * BLK, channels), dtype) for dtype in dtypes],
        in_specs=[pl.BlockSpec(memory_space=pltpu.SMEM)]
        + [pl.BlockSpec(memory_space=pl.ANY)] * (len(codes) + 4),
        out_specs=[pl.BlockSpec(memory_space=pltpu.VMEM)] * len(dtypes),
        scratch_shapes=[
            pltpu.VMEM((slots, BLK, BLK), jnp.int32),
            pltpu.VMEM((slots, BLK, channels), jnp.bfloat16),
            pltpu.VMEM((slots, BLK, channels), jnp.bfloat16),
            pltpu.VMEM((2, NB_DEV * BLK, channels), jnp.float32),
            pltpu.SemaphoreType.DMA((3, slots)),
        ],
        cost_estimate=pl.CostEstimate(flops=flops, bytes_accessed=moved, transcendentals=0),
        compiler_params=pltpu.CompilerParams(vmem_limit_bytes=VMEM_GRANT),
        name="tile_products",
    )(meta, *codes, *blocks)


def project_kernel(chan_ref, p0, p1, p2, p3, enc_mix, dec_proj, node_embed, hidden, node_grad):
    chan = chan_ref[0]
    mixed = None
    for by, piece in enumerate((p0, p1, p2, p3)):
        rows = pl.ds(pl.multiple_of((chan ^ by) * 256, 256), 256)
        left = jnp.dot(piece[0], enc_mix[rows, :], preferred_element_type=jnp.float32)
        right = jnp.dot(piece[1], dec_proj[rows, :], preferred_element_type=jnp.float32)
        mixed, grad = (left, right) if mixed is None else (mixed + left, grad + right)
    hidden[...] = (node_embed[...].astype(jnp.float32) + mixed / (1.0 + jnp.exp(-mixed))).astype(hidden.dtype)
    node_grad[...] = grad.astype(node_grad.dtype)


def project(chan, pieces, enc_mix, dec_proj, node_embed):
    rows, channels = node_embed.shape
    vmem = pl.BlockSpec(memory_space=pltpu.VMEM)
    return pl.pallas_call(
        project_kernel,
        out_shape=[jax.ShapeDtypeStruct((rows, channels), jnp.bfloat16)] * 2,
        in_specs=[pl.BlockSpec(memory_space=pltpu.SMEM)] + [vmem] * 7,
        out_specs=[vmem] * 2,
        cost_estimate=pl.CostEstimate(
            flops=4 * rows * CHAN * channels * channels,
            bytes_accessed=4 * CHAN * rows * channels * 4,
            transcendentals=rows * channels,
        ),
        compiler_params=pltpu.CompilerParams(vmem_limit_bytes=VMEM_GRANT),
        name="project",
    )(chan.reshape(1), *pieces, enc_mix, dec_proj, node_embed)


def near_step(band):
    return 1 - 2 * (band // 2 % 2)


def one_device(
    cells_next, node_embed, enc_mix, out_cotangent, decoded_saved, dec_proj, tile_source, tile_codes
):
    bands = lax.axis_size("band")
    band = lax.axis_index("band")
    chan = lax.axis_index("chan")
    core = band % 2
    tile_scale = (3.0 / (K * BLK)) ** 0.5 / 128.0
    channels = cells_next.shape[1]
    go = functools.partial(permute, bands=bands)
    codes = tile_codes.reshape(TILES, BLK, BLK)
    cells = cells_next.reshape(CB_DEV, BLK, channels)
    cotangent = out_cotangent.reshape(CB_DEV, BLK, channels)
    quarter = SIDE // CHAN

    cells_sib = go(cells, lambda b, c: (b ^ 1, c))
    cotangent_sib = go(cotangent, lambda b, c: (b ^ 1, c))

    place = jnp.stack([band, chan]).astype(jnp.int32)
    give_codes, keep_codes = pick_tiles(place, tile_source.T, codes, ((0, "mirrored"), (1, "mirrored")))
    give_extra, keep_extra, far_codes = pick_tiles(place, tile_source.T, codes, ((0, "own"), (1, "own"), (2, "all")))

    def mirrored(c):
        return CHAN - 1 - c

    give_to = lambda b: b - 2 * near_step(b)
    keep_to = lambda b: b ^ 2

    give_codes = go(give_codes, lambda b, c: (give_to(b), mirrored(c)))
    keep_codes = go(keep_codes, lambda b, c: (keep_to(b), mirrored(c)))
    far_codes = go(far_codes, lambda b, c: (b - 2 * far_step(b), c))

    at_end = (chan == 0) | (chan == CHAN - 1)

    def along_chan(x, extra, reader):
        one, two = (go(x, lambda b, c, by=by: (b, c ^ by)) for by in (1, 2))
        three = go(
            jnp.where(at_end, extra, x),
            lambda b, c: (reader(b) if c in (0, CHAN - 1) else b, mirrored(c)),
        )
        return [x, one, two, three]

    give_codes = along_chan(give_codes, give_extra, give_to)
    keep_codes = along_chan(keep_codes, keep_extra, keep_to)

    def over_chan(x):
        return [x] + [go(x, lambda b, c, by=by: (b, c ^ by)) for by in range(1, CHAN)]

    half = decoded_saved.shape[0] // 2
    dec_first = go(decoded_saved[:half], lambda b, c: (b, c ^ 2))
    cot_pair = go(out_cotangent, lambda b, c: (b, c ^ 1))
    dec_second = go(lax.optimization_barrier(decoded_saved)[half:], lambda b, c: (b, c ^ 2))

    near = near_step(band)
    far = far_step_traced(core)
    readers = band + jnp.array([2, -2, 0, 0], jnp.int32) * near + jnp.array([0, 0, 2, 0], jnp.int32) * far
    offsets = jnp.array([-1, 1, 0, 0], jnp.int32) * near + jnp.array([0, 0, -1, 0], jnp.int32) * far
    tile, block = slot_table(tile_source, readers, offsets)

    slots = jnp.arange(SIDE, dtype=jnp.int32)

    def meta_of(row, index):
        node = jnp.where(tile[row] < 0, NB_DEV, tile[row] // K)
        own = (block[row] // CB_DEV == core).astype(jnp.int32)
        return jnp.stack([node, own, block[row] % CB_DEV, index, (slots // quarter) ^ chan])

    def pieces_meta(row):
        return meta_of(row, slots % quarter)

    blocks = (cells, cells_sib, cotangent, cotangent_sib)
    piece_group = [[(tuple(range(CHAN)), 0, SIDE)]]
    near_meta = jnp.concatenate([meta_of(2, slots)[:, :CAP], meta_of(3, jnp.maximum(tile[3], 0))], axis=1)
    far_part, own_part = tile_products(
        near_meta, [far_codes, codes], blocks, [[((0,), 0, CAP)], [((1,), CAP, SIDE)]], [jnp.bfloat16, jnp.float32]
    )
    got_far = go(far_part, lambda b, c: (b + 2 * far_step(b), c))
    (give_part,) = tile_products(pieces_meta(1), give_codes, blocks, piece_group, [jnp.bfloat16])
    got_give = go(give_part, lambda b, c: (b - 4 * near_step(b), c))
    (keep_part,) = tile_products(pieces_meta(0), keep_codes, blocks, piece_group, [jnp.float32])
    crossing = (keep_part + got_give.astype(jnp.float32)).astype(jnp.bfloat16)
    got_keep = go(crossing, lambda b, c: (b ^ 2, c))
    summed = own_part + got_keep.astype(jnp.float32) + got_far.astype(jnp.float32)
    aggregates = (summed * tile_scale).astype(jnp.bfloat16)
    pieces = over_chan(aggregates)
    hidden_nodes, node_grad = project(chan, pieces, enc_mix, dec_proj, node_embed)

    w_dec_grad = projection_gradient(go, out_cotangent, decoded_saved, cot_pair, (dec_first, dec_second), bands)
    return (hidden_nodes, node_grad, w_dec_grad)


def far_step_traced(core):
    return 2 - 4 * core


def projection_gradient(go, cot, dec, cot_pair, dec_pair, bands):
    band, chan = lax.axis_index("band"), lax.axis_index("chan")
    along = bands // 16
    x, y, zh, core = band // (4 * along), band // along % 4, band // 2 % 2, band % 2
    channels = cot.shape[1]
    cells_total = cot.shape[0] * bands
    rows = channels // 16

    def outer(left, right):
        return lax.dot_general(left, right, (((0,), (0,)), ((), ())), preferred_element_type=jnp.float32)

    half = cot.shape[0] // 2
    first = outer(cot, dec)
    third = lax.optimization_barrier(outer(cot[:half], dec_pair[0]))
    second = outer(cot_pair, dec)
    fourth = lax.optimization_barrier(outer(cot_pair[:half], dec_pair[0]))
    third = third + outer(cot[half:], dec_pair[1])
    fourth = fourth + outer(cot_pair[half:], dec_pair[1])
    whole = jnp.stack([first, second, third, fourth])
    halves = whole.reshape(4, 8, 2, rows, channels)
    own = lax.dynamic_index_in_dim(halves, core, 2, keepdims=False)
    other = lax.dynamic_index_in_dim(halves, 1 - core, 2, keepdims=False).astype(jnp.bfloat16)
    own = own + go(other, lambda b, c: (b ^ 1, c)).astype(jnp.float32)

    def take(i):
        return lax.dynamic_index_in_dim(own, i, 0, keepdims=False)

    share = take(x ^ chan)
    for by in range(1, 4):
        sent = take(x ^ by ^ chan).astype(jnp.bfloat16)
        share = share + go(sent, lambda b, c: (b ^ (by * 4 * along), c)).astype(jnp.float32)

    own = share.reshape(4, 2, rows, channels)
    share = take(y)
    for by in range(1, 4):
        share = share + go(take(y ^ by), lambda b, c: (b ^ (by * 4), c))

    def home(b, c):
        at_x, rest = b // 16, b % 16
        return (2 * (c // 2) + at_x % 2) * 16 + rest, c % 2 + 2 * (at_x // 2)

    def home_across(b, c):
        return home(b ^ 2, c)

    own = share
    return (go(take(zh), home) + go(take(1 - zh), home_across)) * cells_total ** (-0.5)


def solution(mesh):
    in_specs = (
        P("band", "chan"),
        P("band", "chan"),
        P(None, "chan"),
        P("band", "chan"),
        P("band", "chan"),
        P(None, "chan"),
        P(),
        P("band", None, None, None),
    )
    out_specs = (P("band", "chan"), P("band", "chan"), P("band", "chan"))
    return jax.shard_map(one_device, mesh=mesh, in_specs=in_specs, out_specs=out_specs, check_vma=False)
```

```python
import functools

import jax
import jax.numpy as jnp
from jax import lax
from jax.experimental import pallas as pl
from jax.experimental.pallas import tpu as pltpu
from jax.sharding import PartitionSpec as P


BLK = 128
K = 16
CB_DEV = 16
NB_DEV = 2
CAP = 8
CHAN = 4
TILES = NB_DEV * K
PAIR_BLOCKS = 2 * CB_DEV
SIDE = 2 * CAP
VMEM_GRANT = 12 * 2**20


def permute(x, move, bands):
    pairs = []
    for band in range(bands):
        for chan in range(CHAN):
            to_band, to_chan = move(band, chan)
            if 0 <= to_band < bands and 0 <= to_chan < CHAN:
                pairs.append((band * CHAN + chan, to_band * CHAN + to_chan))
    return lax.ppermute(x, ("band", "chan"), pairs)


def far_step(band):
    return 2 if band % 2 == 0 else -2


def slot_table(tile_source, readers, offsets):
    bands = tile_source.shape[0] // NB_DEV
    rows = tile_source.reshape(bands, TILES)[jnp.clip(readers, 0, bands - 1)]
    hit = (rows // PAIR_BLOCKS - (readers // 2)[:, None]) == offsets[:, None]
    earlier = jnp.tril(jnp.ones((TILES, TILES), jnp.int32), -1)
    rank = jnp.sum(hit.astype(jnp.int32)[:, None, :] * earlier[None], axis=2)
    code = (jnp.arange(TILES, dtype=jnp.int32) * PAIR_BLOCKS)[None] + rows % PAIR_BLOCKS + 1
    chosen = hit[:, None, :] & (rank[:, None, :] == jnp.arange(SIDE, dtype=jnp.int32)[None, :, None])
    packed = jnp.sum(jnp.where(chosen, code[:, None, :], 0), axis=2) - 1
    tile = jnp.where(packed < 0, -1, packed // PAIR_BLOCKS)
    block = jnp.where(packed < 0, 0, packed % PAIR_BLOCKS)
    return tile, block


def pick_kernel(picks, place, rows, codes, *refs):
    outs, (listed, sems) = refs[:-2], refs[-2:]
    band, chan = place[0], place[1]
    chip = band // 2
    near = 1 - 2 * (chip % 2)
    far = 2 - 4 * (band % 2)
    starts = {"mirrored": (CHAN - 1 - chan) * (SIDE // CHAN), "own": chan * (SIDE // CHAN), "all": 0}
    for i in range(3 * SIDE):
        listed[i] = 0

    def sort(tile, counts):
        offset = rows[tile % K, band * NB_DEV + tile // K] // PAIR_BLOCKS - chip
        after = []
        for kind, (wanted, count) in enumerate(zip((-near, near, -far), counts)):
            hit = offset == wanted

            @pl.when(hit & (count < SIDE))
            def _(kind=kind, count=count):
                listed[kind * SIDE + count] = tile

            after.append(count + hit.astype(jnp.int32))
        return tuple(after)

    zero = jnp.int32(0)
    lax.fori_loop(0, TILES, sort, (zero, zero, zero))
    copies = []
    for out, (kind, which) in zip(outs, picks):
        for i in range(out.shape[0]):
            tile = listed[kind * SIDE + starts[which] + i]
            copies.append(pltpu.make_async_copy(codes.at[tile], out.at[i], sems.at[len(copies)]))
            copies[-1].start()
    for copy in copies:
        copy.wait()


def pick_tiles(place, rows, codes, picks):
    counts = [CAP if which == "all" else SIDE // CHAN for _, which in picks]
    smem = pl.BlockSpec(memory_space=pltpu.SMEM)
    return pl.pallas_call(
        functools.partial(pick_kernel, picks),
        out_shape=[jax.ShapeDtypeStruct((count, BLK, BLK), codes.dtype) for count in counts],
        in_specs=[smem, smem, pl.BlockSpec(memory_space=pl.ANY)],
        out_specs=[pl.BlockSpec(memory_space=pltpu.VMEM)] * len(counts),
        scratch_shapes=[pltpu.SMEM((3 * SIDE,), jnp.int32), pltpu.SemaphoreType.DMA((sum(counts),))],
        cost_estimate=pl.CostEstimate(flops=10**8, bytes_accessed=2 * sum(counts) * BLK * BLK * 4, transcendentals=0),
        compiler_params=pltpu.CompilerParams(vmem_limit_bytes=VMEM_GRANT),
        name="pick_tiles",
    )(place, rows, codes)


def products_kernel(groups, n_codes, *refs):
    meta = refs[0]
    codes = refs[1 : 1 + n_codes]
    cells_own, cells_sib, cot_own, cot_sib = refs[1 + n_codes : 5 + n_codes]
    outs = refs[5 + n_codes : 5 + n_codes + len(groups)]
    code_buf, cell_buf, cot_buf, total, sems = refs[5 + n_codes + len(groups) :]
    for parts in groups:
        for operands, first, count in parts:

            def begin(i, carry, first=first, operands=operands):
                slot = first + i
                for operand in operands:

                    @pl.when((meta[4, slot] == operand) | (len(operands) == 1))
                    def _(operand=operand):
                        pltpu.make_async_copy(
                            codes[operand].at[meta[3, slot]], code_buf.at[slot], sems.at[0, slot]
                        ).start()

                local = meta[2, slot]

                @pl.when(meta[1, slot] == 1)
                def _():
                    pltpu.make_async_copy(cells_own.at[local], cell_buf.at[slot], sems.at[1, slot]).start()
                    pltpu.make_async_copy(cot_own.at[local], cot_buf.at[slot], sems.at[2, slot]).start()

                @pl.when(meta[1, slot] != 1)
                def _():
                    pltpu.make_async_copy(cells_sib.at[local], cell_buf.at[slot], sems.at[1, slot]).start()
                    pltpu.make_async_copy(cot_sib.at[local], cot_buf.at[slot], sems.at[2, slot]).start()

                return carry

            lax.fori_loop(0, count, begin, 0)

    for out, parts in zip(outs, groups):
        total[...] = jnp.zeros_like(total)
        first = parts[0][1]
        slots = sum(count for _, _, count in parts)

        def step(i, carry, first=first):
            enc_rows, dec_rows = [[], []], [[], []]
            base = first + i * 4
            for inner in range(4):
                slot = base + inner
                pltpu.make_async_copy(codes[0].at[0], code_buf.at[slot], sems.at[0, slot]).wait()
                pltpu.make_async_copy(cells_own.at[0], cell_buf.at[slot], sems.at[1, slot]).wait()
                pltpu.make_async_copy(cot_own.at[0], cot_buf.at[slot], sems.at[2, slot]).wait()
                words = code_buf[slot]
                enc = ((words & 255) - 128).astype(jnp.float32)
                dec = ((words >> 8) - 128).astype(jnp.float32)
                for node in range(NB_DEV):
                    keep = (meta[0, slot] == node).astype(jnp.float32)
                    enc_rows[node].append((enc * keep).astype(jnp.bfloat16))
                    dec_rows[node].append((dec * keep).astype(jnp.bfloat16))
            wide = [
                jnp.concatenate([jnp.concatenate(line, axis=1) for line in both], axis=0)
                for both in (enc_rows, dec_rows)
            ]
            cells = cell_buf[pl.ds(base, 4)].reshape(4 * BLK, -1)
            cots = cot_buf[pl.ds(base, 4)].reshape(4 * BLK, -1)
            total[0] += jnp.dot(wide[0], cells, preferred_element_type=jnp.float32)
            total[1] += jnp.dot(wide[1], cots, preferred_element_type=jnp.float32)
            return carry

        lax.fori_loop(0, slots // 4, step, 0)
        out[...] = total[...].astype(out.dtype)


def tile_products(meta, codes, blocks, groups, dtypes):
    slots = meta.shape[1]
    channels = blocks[0].shape[-1]
    flops = slots * 4 * BLK * BLK * channels
    moved = slots * (BLK * BLK * 4 + 2 * BLK * channels * 2)
    return pl.pallas_call(
        functools.partial(products_kernel, groups, len(codes)),
        out_shape=[jax.ShapeDtypeStruct((2, NB_DEV * BLK, channels), dtype) for dtype in dtypes],
        in_specs=[pl.BlockSpec(memory_space=pltpu.SMEM)]
        + [pl.BlockSpec(memory_space=pl.ANY)] * (len(codes) + 4),
        out_specs=[pl.BlockSpec(memory_space=pltpu.VMEM)] * len(dtypes),
        scratch_shapes=[
            pltpu.VMEM((slots, BLK, BLK), jnp.int32),
            pltpu.VMEM((slots, BLK, channels), jnp.bfloat16),
            pltpu.VMEM((slots, BLK, channels), jnp.bfloat16),
            pltpu.VMEM((2, NB_DEV * BLK, channels), jnp.float32),
            pltpu.SemaphoreType.DMA((3, slots)),
        ],
        cost_estimate=pl.CostEstimate(flops=flops, bytes_accessed=moved, transcendentals=0),
        compiler_params=pltpu.CompilerParams(vmem_limit_bytes=VMEM_GRANT),
        name="tile_products",
    )(meta, *codes, *blocks)


def project_kernel(chan_ref, p0, p1, p2, p3, enc_mix, dec_proj, node_embed, hidden, node_grad):
    chan = chan_ref[0]
    mixed = None
    for by, piece in enumerate((p0, p1, p2, p3)):
        rows = pl.ds(pl.multiple_of((chan ^ by) * 256, 256), 256)
        left = jnp.dot(piece[0], enc_mix[rows, :], preferred_element_type=jnp.float32)
        right = jnp.dot(piece[1], dec_proj[rows, :], preferred_element_type=jnp.float32)
        mixed, grad = (left, right) if mixed is None else (mixed + left, grad + right)
    hidden[...] = (node_embed[...].astype(jnp.float32) + mixed / (1.0 + jnp.exp(-mixed))).astype(hidden.dtype)
    node_grad[...] = grad.astype(node_grad.dtype)


def project(chan, pieces, enc_mix, dec_proj, node_embed):
    rows, channels = node_embed.shape
    vmem = pl.BlockSpec(memory_space=pltpu.VMEM)
    return pl.pallas_call(
        project_kernel,
        out_shape=[jax.ShapeDtypeStruct((rows, channels), jnp.bfloat16)] * 2,
        in_specs=[pl.BlockSpec(memory_space=pltpu.SMEM)] + [vmem] * 7,
        out_specs=[vmem] * 2,
        cost_estimate=pl.CostEstimate(
            flops=4 * rows * CHAN * channels * channels,
            bytes_accessed=4 * CHAN * rows * channels * 4,
            transcendentals=rows * channels,
        ),
        compiler_params=pltpu.CompilerParams(vmem_limit_bytes=VMEM_GRANT),
        name="project",
    )(chan.reshape(1), *pieces, enc_mix, dec_proj, node_embed)


def near_step(band):
    return 1 - 2 * (band // 2 % 2)


def one_device(
    cells_next, node_embed, enc_mix, out_cotangent, decoded_saved, dec_proj, tile_source, tile_codes
):
    bands = lax.axis_size("band")
    band = lax.axis_index("band")
    chan = lax.axis_index("chan")
    core = band % 2
    tile_scale = (3.0 / (K * BLK)) ** 0.5 / 128.0
    channels = cells_next.shape[1]
    go = functools.partial(permute, bands=bands)
    codes = tile_codes.reshape(TILES, BLK, BLK)
    cells = cells_next.reshape(CB_DEV, BLK, channels)
    cotangent = out_cotangent.reshape(CB_DEV, BLK, channels)
    quarter = SIDE // CHAN

    cells_sib = go(cells, lambda b, c: (b ^ 1, c))
    cotangent_sib = go(cotangent, lambda b, c: (b ^ 1, c))

    place = jnp.stack([band, chan]).astype(jnp.int32)
    give_codes, keep_codes = pick_tiles(place, tile_source.T, codes, ((0, "mirrored"), (1, "mirrored")))
    give_extra, keep_extra, far_codes = pick_tiles(place, tile_source.T, codes, ((0, "own"), (1, "own"), (2, "all")))

    def mirrored(c):
        return CHAN - 1 - c

    give_to = lambda b: b - 2 * near_step(b)
    keep_to = lambda b: b ^ 2

    give_codes = go(give_codes, lambda b, c: (give_to(b), mirrored(c)))
    keep_codes = go(keep_codes, lambda b, c: (keep_to(b), mirrored(c)))
    far_codes = go(far_codes, lambda b, c: (b - 2 * far_step(b), c))

    at_end = (chan == 0) | (chan == CHAN - 1)

    def along_chan(x, extra, reader):
        one, two = (go(x, lambda b, c, by=by: (b, c ^ by)) for by in (1, 2))
        three = go(
            jnp.where(at_end, extra, x),
            lambda b, c: (reader(b) if c in (0, CHAN - 1) else b, mirrored(c)),
        )
        return [x, one, two, three]

    give_codes = along_chan(give_codes, give_extra, give_to)
    keep_codes = along_chan(keep_codes, keep_extra, keep_to)

    def over_chan(x):
        return [x] + [go(x, lambda b, c, by=by: (b, c ^ by)) for by in range(1, CHAN)]

    half = decoded_saved.shape[0] // 2
    dec_first = go(decoded_saved[:half], lambda b, c: (b, c ^ 2))
    cot_first = go(lax.optimization_barrier(out_cotangent)[:half], lambda b, c: (b, c ^ 1))
    cot_second = go(lax.optimization_barrier(out_cotangent)[half:], lambda b, c: (b, c ^ 1))
    dec_second = go(lax.optimization_barrier(decoded_saved)[half:], lambda b, c: (b, c ^ 2))

    near = near_step(band)
    far = far_step_traced(core)
    readers = band + jnp.array([2, -2, 0, 0], jnp.int32) * near + jnp.array([0, 0, 2, 0], jnp.int32) * far
    offsets = jnp.array([-1, 1, 0, 0], jnp.int32) * near + jnp.array([0, 0, -1, 0], jnp.int32) * far
    tile, block = slot_table(tile_source, readers, offsets)

    slots = jnp.arange(SIDE, dtype=jnp.int32)

    def meta_of(row, index):
        node = jnp.where(tile[row] < 0, NB_DEV, tile[row] // K)
        own = (block[row] // CB_DEV == core).astype(jnp.int32)
        return jnp.stack([node, own, block[row] % CB_DEV, index, (slots // quarter) ^ chan])

    def pieces_meta(row):
        return meta_of(row, slots % quarter)

    blocks = (cells, cells_sib, cotangent, cotangent_sib)
    piece_group = [[(tuple(range(CHAN)), 0, SIDE)]]
    near_meta = jnp.concatenate([meta_of(2, slots)[:, :CAP], meta_of(3, jnp.maximum(tile[3], 0))], axis=1)
    far_part, own_part = tile_products(
        near_meta, [far_codes, codes], blocks, [[((0,), 0, CAP)], [((1,), CAP, SIDE)]], [jnp.bfloat16, jnp.float32]
    )
    got_far = go(far_part, lambda b, c: (b + 2 * far_step(b), c))
    (give_part,) = tile_products(pieces_meta(1), give_codes, blocks, piece_group, [jnp.bfloat16])
    got_give = go(give_part, lambda b, c: (b - 4 * near_step(b), c))
    (keep_part,) = tile_products(pieces_meta(0), keep_codes, blocks, piece_group, [jnp.float32])
    crossing = (keep_part + got_give.astype(jnp.float32)).astype(jnp.bfloat16)
    got_keep = go(crossing, lambda b, c: (b ^ 2, c))
    summed = own_part + got_keep.astype(jnp.float32) + got_far.astype(jnp.float32)
    aggregates = (summed * tile_scale).astype(jnp.bfloat16)
    pieces = over_chan(aggregates)
    hidden_nodes, node_grad = project(chan, pieces, enc_mix, dec_proj, node_embed)

    w_dec_grad = projection_gradient(go, out_cotangent, decoded_saved, (cot_first, cot_second), (dec_first, dec_second), bands)
    return (hidden_nodes, node_grad, w_dec_grad)


def far_step_traced(core):
    return 2 - 4 * core


def projection_gradient(go, cot, dec, cot_pair, dec_pair, bands):
    band, chan = lax.axis_index("band"), lax.axis_index("chan")
    along = bands // 16
    x, y, zh, core = band // (4 * along), band // along % 4, band // 2 % 2, band % 2
    channels = cot.shape[1]
    cells_total = cot.shape[0] * bands
    rows = channels // 16

    def outer(left, right):
        return lax.dot_general(left, right, (((0,), (0,)), ((), ())), preferred_element_type=jnp.float32)

    half = cot.shape[0] // 2
    first = outer(cot, dec)
    early = lax.optimization_barrier(
        (outer(cot_pair[0], dec[:half]), outer(cot[:half], dec_pair[0]), outer(cot_pair[0], dec_pair[0]))
    )
    second = early[0] + outer(cot_pair[1], dec[half:])
    third = early[1] + outer(cot[half:], dec_pair[1])
    fourth = early[2] + outer(cot_pair[1], dec_pair[1])
    whole = jnp.stack([first, second, third, fourth])
    halves = whole.reshape(4, 8, 2, rows, channels)
    own = lax.dynamic_index_in_dim(halves, core, 2, keepdims=False)
    other = lax.dynamic_index_in_dim(halves, 1 - core, 2, keepdims=False).astype(jnp.bfloat16)
    own = own + go(other, lambda b, c: (b ^ 1, c)).astype(jnp.float32)

    def take(i):
        return lax.dynamic_index_in_dim(own, i, 0, keepdims=False)

    share = take(x ^ chan)
    for by in range(1, 4):
        sent = take(x ^ by ^ chan).astype(jnp.bfloat16)
        share = share + go(sent, lambda b, c: (b ^ (by * 4 * along), c)).astype(jnp.float32)

    own = share.reshape(4, 2, rows, channels)
    share = take(y)
    for by in range(1, 4):
        share = share + go(take(y ^ by), lambda b, c: (b ^ (by * 4), c))

    def home(b, c):
        at_x, rest = b // 16, b % 16
        return (2 * (c // 2) + at_x % 2) * 16 + rest, c % 2 + 2 * (at_x // 2)

    def home_across(b, c):
        return home(b ^ 2, c)

    own = share
    return (go(take(zh), home) + go(take(1 - zh), home_across)) * cells_total ** (-0.5)


def solution(mesh):
    in_specs = (
        P("band", "chan"),
        P("band", "chan"),
        P(None, "chan"),
        P("band", "chan"),
        P("band", "chan"),
        P(None, "chan"),
        P(),
        P("band", None, None, None),
    )
    out_specs = (P("band", "chan"), P("band", "chan"), P("band", "chan"))
    return jax.shard_map(one_device, mesh=mesh, in_specs=in_specs, out_specs=out_specs, check_vma=False)
```
